32 devices in a mesh: rows: 16 (over z, y, x), rhs: 2 (over core).
Axes of the slice: x: 2, y: 2, z: 4, core: 2. Of those that a mesh axis runs over, the one named last changes fastest.
Arguments:
- rhs: float32 [2, 8192, 4096], P(None, 'rows', 'rhs'), may hold values from -8 to 8
- factor: bfloat16 [2, 8192, 4, 512], P(None, 'rows', None, 'rhs'), may hold values from -0.125 to 0.125
- inverses: float32 [4, 512, 512], replicated, may hold values from -1 to 1, as said below
Outputs:
- state: float32 [2, 8192, 4096], P(None, 'rows', 'rhs')
The draws below stay inside these ranges and needn't reach their ends.
Inputs may be any that keep to these rules, and one draw needn't show every extreme that they name: Each inverses[p] is unit lower triangular: ones on the diagonal, zeros above it.
All inputs are finite; a program needn't handle non-finite values.
Results may differ from the reference program's by a relative error of at most 0.003.
Values may be sent and summed in bfloat16 or wider, within the bound.
A program may use at most 128 MiB of HBM per device.

```python
import jax
import jax.numpy as jnp
from jax import lax

TILE = 512
PANELS = 4
NRHS = 4096
CYC = 2
WIDTH = 8192
N_ROWS = 16


def draw_inverses(key, part):
    values = jax.random.normal(key, (PANELS, TILE, TILE), jnp.float32)
    values = jnp.clip(values, -4.0, 4.0) * TILE ** (-0.5)
    return jnp.tril(values, -1) + jnp.eye(TILE, dtype=jnp.float32)[None]


def level_of(rng, shape, cuts, low, high):
    loudness, own = 1.0, jax.random.fold_in(rng, 6)
    for axis_at, shards_of in cuts:
        steps = jnp.exp(jax.random.uniform(jax.random.fold_in(own, axis_at), (shards_of,), jnp.float32, low / len(cuts), high / len(cuts)))
        loudness = loudness * jnp.repeat(steps, shape[axis_at] // shards_of).reshape([-1 if axis == axis_at else 1 for axis in range(len(shape))])
    return loudness


def bell_draw(key, dims, scale, reach, split=(), kind=jnp.bfloat16):
    result = jax.random.normal(key, dims, jnp.float32) * scale
    if len(split) > 0:
        result = level_of(key, dims, split, -0.22, 0.18) * result
    return jnp.clip(result, min=-reach, max=reach).astype(kind)


def setup_inputs(seed: int = 0) -> dict:
    keys = jax.random.split(jax.random.key(seed), 4)
    rhs = bell_draw(keys[0], (CYC, WIDTH, NRHS), 1.0, 8.0, ((1, 16), (2, 2)), jnp.float32)
    factor = bell_draw(keys[1], (CYC, WIDTH, PANELS, TILE), (PANELS * TILE) ** -0.5, 0.125, ((1, 16), (3, 2)))
    inverses = draw_inverses(jax.random.fold_in(keys[3], 71), 0)
    return {"rhs": rhs, "factor": factor, "inverses": inverses}


def reference(rhs, factor, inverses):
    cycles = rhs.shape[0]
    width = rhs.shape[1]
    tile_ids = jnp.arange(cycles, dtype=jnp.int32)[:, None] * N_ROWS + (jnp.arange(width, dtype=jnp.int32) // TILE)[None, :]
    state = rhs
    for panel in range(PANELS):
        pivot = state[0, panel * TILE:(panel + 1) * TILE]
        solved = jnp.dot(inverses[panel], pivot, precision=lax.Precision.HIGHEST)
        sent = lax.optimization_barrier(solved.astype(jnp.bfloat16)).astype(jnp.float32)
        state = state.at[0, panel * TILE:(panel + 1) * TILE].set(solved)
        delta = jnp.einsum("crk,kn->crn", factor[:, :, panel, :].astype(jnp.float32), sent, precision=lax.Precision.HIGHEST)
        state = state - jnp.where((tile_ids > panel)[:, :, None], delta, jnp.float32(0.0))
    return state
```

```python
import functools

import jax
import jax.numpy as jnp
from jax import lax
from jax.experimental import pallas as pl
from jax.experimental.pallas import tpu as pltpu
from jax.sharding import PartitionSpec as P

LAGS = ((0, 2, 4, 6), (0, 0, 3, 5), (0, 2, 2, 5), (0, 0, 2, 2))
LANES = 128


def pick(place, values):
    total = jnp.int32(0)
    for i, v in enumerate(values):
        total = total + jnp.where(place == i, jnp.int32(v), jnp.int32(0))
    return total


def kernel(count, rhs, fac, inv, out, sent, fbuf, ibuf, xbuf,
           f_in, f_send, f_recv, i_in, x_in, x_out,
           own_recv, a_recv, b_recv, dx_recv, dy_recv,
           n1_send, n2_send, up_send, ra_send, rb_send):
    chunks, cycles, tile, lanes = xbuf.shape
    panels = inv.shape[0]
    kpart = fac.shape[1] // panels
    half = tile // 2
    planes = count // panels
    bf16, f32 = jnp.bfloat16, jnp.float32

    me = lax.axis_index("rows")
    core = lax.axis_index("rhs")
    z = me // panels
    c = me % panels
    n1 = c + 1 - 2 * (c % 2)
    n2 = (c + 2) % panels
    base = z * panels
    to_core = {"rows": me, "rhs": 1 - core}
    to_n1 = {"rows": base + n1, "rhs": core}
    to_n2 = {"rows": base + n2, "rhs": core}
    to_up = {"rows": jnp.minimum(me + panels, count - 1), "rhs": core}
    to_down = {"rows": jnp.maximum(me - panels, 0), "rhs": core}
    has_up = z < planes - 1
    has_down = z > 0

    def x_load(j):
        cols = pl.ds(pl.multiple_of(j * lanes, lanes), lanes)
        return pltpu.make_async_copy(rhs.at[:, :, cols], xbuf.at[j], x_in.at[j])

    def x_store(j):
        cols = pl.ds(pl.multiple_of(j * lanes, lanes), lanes)
        return pltpu.make_async_copy(xbuf.at[j], out.at[:, :, cols], x_out.at[j])

    def i_load():
        return pltpu.make_async_copy(inv.at[c], ibuf, i_in)

    def f_parts(cycle, p):
        src = fac.at[pl.ds(cycle * tile, tile), pl.ds(p * kpart, kpart)]
        at = pl.multiple_of(p * 2 * kpart + core * kpart, kpart)
        return src, fbuf.at[pl.ds(cycle * tile, tile), pl.ds(at, kpart)], cycle * panels + p

    def f_local(cycle, p):
        src, dst, at = f_parts(cycle, p)
        return pltpu.make_async_copy(src, dst, f_in.at[at])

    def f_remote(cycle, p):
        src, dst, at = f_parts(cycle, p)
        return pltpu.make_async_remote_copy(src, dst, f_send.at[at], f_recv.at[at], device_id=to_core)

    def f_arrive(cycle, p):
        at = pl.multiple_of(p * 2 * kpart + (1 - core) * kpart, kpart)
        dst = fbuf.at[pl.ds(cycle * tile, tile), pl.ds(at, kpart)]
        src, _, s = f_parts(cycle, p)
        return pltpu.make_async_remote_copy(src, dst, f_send.at[s], f_recv.at[s], device_id=to_core)

    def hop(j, p, start, size, send, recv, to):
        at = pl.multiple_of(p * tile + start, half)
        ref = sent.at[j, pl.ds(at, size)]
        return pltpu.make_async_remote_copy(ref, ref, send.at[j], recv.at[j], device_id=to)

    def own_n1(j):
        return hop(j, c, 0, tile, n1_send, a_recv, to_n1)

    def own_n2(j):
        return hop(j, c, 0, tile, n2_send, b_recv, to_n2)

    def own_up(j):
        return hop(j, c, 0, tile, up_send, own_recv, to_up)

    def relay_a(j):
        return hop(j, n1, half, half, ra_send, dy_recv, to_n2)

    def relay_b(j):
        return hop(j, n2, 0, half, rb_send, dx_recv, to_n1)

    def arrive_a(j):
        return hop(j, n1, 0, tile, n1_send, a_recv, to_n1)

    def arrive_b(j):
        return hop(j, n2, 0, tile, n2_send, b_recv, to_n2)

    def arrive_dx(j):
        return hop(j, panels - 1 - c, 0, half, rb_send, dx_recv, to_n1)

    def arrive_dy(j):
        return hop(j, panels - 1 - c, half, half, ra_send, dy_recv, to_n2)

    @pl.when(z == 0)
    def _():
        i_load().start()

    @pl.loop(0, chunks)
    def _(j):
        x_load(j).start()

    for cycle in range(cycles):
        for p in range(panels):
            f_local(cycle, p).start()

    barrier = pltpu.get_barrier_semaphore()
    for to in (to_core, to_n1, to_n2):
        pl.semaphore_signal(barrier, inc=1, device_id=to)

    @pl.when(has_up)
    def _():
        pl.semaphore_signal(barrier, inc=1, device_id=to_up)

    @pl.when(has_down)
    def _():
        pl.semaphore_signal(barrier, inc=1, device_id=to_down)

    pl.semaphore_wait(barrier, 3 + jnp.where(has_up, 1, 0) + jnp.where(has_down, 1, 0))

    for cycle in range(cycles):
        for p in range(panels):
            f_remote(cycle, p).start()

    def f_wait(cycle):
        for p in range(panels):
            f_local(cycle, p).wait()
            f_arrive(cycle, p).wait_recv()

    def solve(p, j):
        x_load(j).wait()

        @pl.when(j == 0)
        def _():
            i_load().wait()
            if p > 0:
                f_wait(0)

        pivot = xbuf[j, 0]
        if p > 0:
            pivot = pivot - jnp.dot(fbuf[:tile, : p * tile], sent[j, : p * tile], preferred_element_type=f32)
        solved = jnp.dot(ibuf[...], pivot, precision=lax.Precision.HIGHEST, preferred_element_type=f32)
        sent[j, p * tile:(p + 1) * tile] = solved.astype(bf16)
        xbuf[j, 0] = solved

    def event(p, j):
        @pl.when(p == c)
        def _():
            @pl.when(z == 0)
            def _():
                solve(p, j)

            @pl.when(z > 0)
            def _():
                own_up(j).wait_recv()

            own_n1(j).start()
            own_n2(j).start()

            @pl.when(has_up)
            def _():
                own_up(j).start()

        @pl.when(p == n1)
        def _():
            arrive_a(j).wait_recv()
            relay_a(j).start()

        @pl.when(p == n2)
        def _():
            arrive_b(j).wait_recv()
            relay_b(j).start()

        @pl.when(p == panels - 1 - c)
        def _():
            arrive_dx(j).wait_recv()
            arrive_dy(j).wait_recv()

    def update(j):
        @pl.when(j == 0)
        def _():
            f_wait(1)

            @pl.when((z > 0) | (c == 0))
            def _():
                f_wait(0)

        @pl.when(z > 0)
        def _():
            x_load(j).wait()

        @pl.loop(jnp.where(z == 0, 1, 0), cycles)
        def _(cycle):
            rows = pl.ds(pl.multiple_of(cycle * tile, tile), tile)
            delta = jnp.dot(fbuf[rows, :], sent[j], preferred_element_type=f32)
            xbuf[j, cycle] = xbuf[j, cycle] - delta

        x_store(j).start()

    lags = [pick(c, [row[p] for row in LAGS]) for p in range(panels)]
    last = max(max(row) for row in LAGS)
    final = lags[0]
    for lag in lags[1:]:
        final = jnp.maximum(final, lag)

    @pl.loop(0, chunks + last)
    def _(r):
        for p in range(panels):
            j = r - lags[p]

            @pl.when((j >= 0) & (j < chunks))
            def _():
                event(p, j)

        done = r - final

        @pl.when((done >= 0) & (done < chunks))
        def _():
            update(done)

    @pl.loop(0, chunks)
    def _(j):
        own_n1(j).wait_send()
        own_n2(j).wait_send()
        relay_a(j).wait_send()
        relay_b(j).wait_send()

        @pl.when(has_up)
        def _():
            own_up(j).wait_send()

        x_store(j).wait()

    for cycle in range(cycles):
        for p in range(panels):
            f_remote(cycle, p).wait_send()


def local(rhs, factor, inverses):
    count = lax.axis_size("rows")
    cycles, tile, width = rhs.shape
    panels = inverses.shape[0]
    kpart = factor.shape[3]
    chunks = width // LANES
    bf16, f32 = jnp.bfloat16, jnp.float32
    fac = factor.reshape(cycles * tile, panels * kpart)
    dma = lambda n: pltpu.SemaphoreType.DMA((n,))
    return pl.pallas_call(
        functools.partial(kernel, count),
        out_shape=jax.ShapeDtypeStruct(rhs.shape, f32),
        in_specs=[pl.BlockSpec(memory_space=pl.ANY)] * 3,
        out_specs=pl.BlockSpec(memory_space=pl.ANY),
        scratch_shapes=[
            pltpu.VMEM((chunks, panels * tile, LANES), bf16),
            pltpu.VMEM((cycles * tile, panels * tile), bf16),
            pltpu.VMEM((tile, tile), f32),
            pltpu.VMEM((chunks, cycles, tile, LANES), f32),
            dma(cycles * panels), dma(cycles * panels), dma(cycles * panels),
            pltpu.SemaphoreType.DMA, dma(chunks), dma(chunks),
            dma(chunks), dma(chunks), dma(chunks), dma(chunks), dma(chunks),
            dma(chunks), dma(chunks), dma(chunks), dma(chunks), dma(chunks),
        ],
        compiler_params=pltpu.CompilerParams(
            collective_id=0, has_side_effects=True, vmem_limit_bytes=56 << 20
        ),
        name="substitute",
    )(rhs, fac, inverses)


def solution(mesh):
    return jax.shard_map(
        local,
        mesh=mesh,
        in_specs=(P(None, "rows", "rhs"), P(None, "rows", None, "rhs"), P()),
        out_specs=P(None, "rows", "rhs"),
        check_vma=False,
    )
```

```python
import functools

import jax
import jax.numpy as jnp
from jax import lax
from jax.experimental import pallas as pl
from jax.experimental.pallas import tpu as pltpu
from jax.sharding import PartitionSpec as P

LAGS = ((1, 3, 9, 17), (0, 0, 8, 8), (3, 5, 5, 7), (4, 4, 6, 6))
LAGS_UP = ((7, 10, 13, 17), (1, 1, 9, 9), (5, 8, 6, 9), (3, 3, 4, 4))
LANES = 128


def pick(place, values):
    total = jnp.int32(0)
    for i, v in enumerate(values):
        total = total + jnp.where(place == i, jnp.int32(v), jnp.int32(0))
    return total


def split(x):
    high = x.astype(jnp.bfloat16)
    return high, (x - high.astype(jnp.float32)).astype(jnp.bfloat16)


def kernel(count, rhs, fac, inv, out, sent, fbuf, ibuf, xbuf,
           f_in, f_send, f_recv, i_in, x_in, x_out,
           own_recv, a_recv, b_recv, dx_recv, dy_recv,
           n1_send, n2_send, up_send, ra_send, rb_send):
    chunks, cycles, tile, lanes = xbuf.shape
    panels = inv.shape[0]
    kpart = fac.shape[1] // panels
    half = tile // 2
    planes = count // panels
    bf16, f32 = jnp.bfloat16, jnp.float32

    me = lax.axis_index("rows")
    core = lax.axis_index("rhs")
    z = me // panels
    c = me % panels
    n1 = c + 1 - 2 * (c % 2)
    n2 = (c + 2) % panels
    base = z * panels
    to_core = {"rows": me, "rhs": 1 - core}
    to_n1 = {"rows": base + n1, "rhs": core}
    to_n2 = {"rows": base + n2, "rhs": core}
    to_up = {"rows": jnp.minimum(me + panels, count - 1), "rhs": core}
    to_down = {"rows": jnp.maximum(me - panels, 0), "rhs": core}
    has_up = z < planes - 1
    has_down = z > 0

    def x_load(j):
        cols = pl.ds(pl.multiple_of(j * lanes, lanes), lanes)
        return pltpu.make_async_copy(rhs.at[:, :, cols], xbuf.at[j], x_in.at[j])

    def x_store(j):
        cols = pl.ds(pl.multiple_of(j * lanes, lanes), lanes)
        return pltpu.make_async_copy(xbuf.at[j], out.at[:, :, cols], x_out.at[j])

    def i_load():
        return pltpu.make_async_copy(inv.at[c], ibuf, i_in)

    def f_parts(cycle, p):
        src = fac.at[pl.ds(cycle * tile, tile), pl.ds(p * kpart, kpart)]
        at = pl.multiple_of(p * 2 * kpart + core * kpart, kpart)
        return src, fbuf.at[pl.ds(cycle * tile, tile), pl.ds(at, kpart)], cycle * panels + p

    def f_local(cycle, p):
        src, dst, at = f_parts(cycle, p)
        return pltpu.make_async_copy(src, dst, f_in.at[at])

    def f_remote(cycle, p):
        src, dst, at = f_parts(cycle, p)
        return pltpu.make_async_remote_copy(src, dst, f_send.at[at], f_recv.at[at], device_id=to_core)

    def f_arrive(cycle, p):
        at = pl.multiple_of(p * 2 * kpart + (1 - core) * kpart, kpart)
        dst = fbuf.at[pl.ds(cycle * tile, tile), pl.ds(at, kpart)]
        src, _, s = f_parts(cycle, p)
        return pltpu.make_async_remote_copy(src, dst, f_send.at[s], f_recv.at[s], device_id=to_core)

    def hop(j, p, start, size, send, recv, to):
        at = pl.multiple_of(p * tile + start, half)
        ref = sent.at[j, pl.ds(at, size)]
        return pltpu.make_async_remote_copy(ref, ref, send.at[j], recv.at[j], device_id=to)

    def own_n1(j):
        return hop(j, c, 0, tile, n1_send, a_recv, to_n1)

    def own_n2(j):
        return hop(j, c, 0, tile, n2_send, b_recv, to_n2)

    def own_up(j):
        return hop(j, c, 0, tile, up_send, own_recv, to_up)

    def relay_a(j):
        return hop(j, n1, half, half, ra_send, dy_recv, to_n2)

    def relay_b(j):
        return hop(j, n2, 0, half, rb_send, dx_recv, to_n1)

    def arrive_a(j):
        return hop(j, n1, 0, tile, n1_send, a_recv, to_n1)

    def arrive_b(j):
        return hop(j, n2, 0, tile, n2_send, b_recv, to_n2)

    def arrive_dx(j):
        return hop(j, panels - 1 - c, 0, half, rb_send, dx_recv, to_n1)

    def arrive_dy(j):
        return hop(j, panels - 1 - c, half, half, ra_send, dy_recv, to_n2)

    @pl.when(z == 0)
    def _():
        i_load().start()

    @pl.loop(0, chunks)
    def _(j):
        x_load(j).start()

    for cycle in range(cycles):
        for p in range(panels):
            f_local(cycle, p).start()

    barrier = pltpu.get_barrier_semaphore()
    for to in (to_core, to_n1, to_n2):
        pl.semaphore_signal(barrier, inc=1, device_id=to)

    @pl.when(has_up)
    def _():
        pl.semaphore_signal(barrier, inc=1, device_id=to_up)

    @pl.when(has_down)
    def _():
        pl.semaphore_signal(barrier, inc=1, device_id=to_down)

    pl.semaphore_wait(barrier, 3 + jnp.where(has_up, 1, 0) + jnp.where(has_down, 1, 0))

    for cycle in range(cycles):
        for p in range(panels):
            f_remote(cycle, p).start()

    def f_wait(cycle):
        for p in range(panels):
            f_local(cycle, p).wait()
            f_arrive(cycle, p).wait_recv()

    def solve(p, j):
        x_load(j).wait()

        @pl.when(j == 0)
        def _():
            i_load().wait()
            if p > 0:
                f_wait(0)

        pivot = xbuf[j, 0]
        if p > 0:
            pivot = pivot - jnp.dot(fbuf[:tile, : p * tile], sent[j, : p * tile], preferred_element_type=f32)
        inv_high, inv_low = split(ibuf[...])
        high, low = split(pivot)
        solved = (
            jnp.dot(inv_low, high, preferred_element_type=f32)
            + jnp.dot(inv_high, low, preferred_element_type=f32)
            + jnp.dot(inv_high, high, preferred_element_type=f32)
        )
        sent[j, p * tile:(p + 1) * tile] = solved.astype(bf16)
        xbuf[j, 0] = solved

    def event(p, j):
        @pl.when(p == c)
        def _():
            @pl.when(z == 0)
            def _():
                solve(p, j)

            @pl.when(z > 0)
            def _():
                own_up(j).wait_recv()

            own_n1(j).start()
            own_n2(j).start()

            @pl.when(has_up)
            def _():
                own_up(j).start()

        @pl.when(p == n1)
        def _():
            arrive_a(j).wait_recv()
            relay_a(j).start()

        @pl.when(p == n2)
        def _():
            arrive_b(j).wait_recv()
            relay_b(j).start()

        @pl.when(p == panels - 1 - c)
        def _():
            arrive_dx(j).wait_recv()
            arrive_dy(j).wait_recv()

    def update(j):
        @pl.when(j == 0)
        def _():
            f_wait(1)

            @pl.when((z > 0) | (c == 0))
            def _():
                f_wait(0)

        @pl.when(z > 0)
        def _():
            x_load(j).wait()

        @pl.loop(jnp.where(z == 0, 1, 0), cycles)
        def _(cycle):
            rows = pl.ds(pl.multiple_of(cycle * tile, tile), tile)
            delta = jnp.dot(fbuf[rows, :], sent[j], preferred_element_type=f32)
            xbuf[j, cycle] = xbuf[j, cycle] - delta

        x_store(j).start()

    lags = [
        jnp.where(z == 0, pick(c, [row[p] for row in LAGS]), pick(c, [row[p] for row in LAGS_UP]))
        for p in range(panels)
    ]
    last = max(max(row) for row in LAGS + LAGS_UP)
    final = lags[0]
    for lag in lags[1:]:
        final = jnp.maximum(final, lag)

    @pl.loop(0, chunks + last)
    def _(r):
        for p in range(panels):
            j = r - lags[p]

            @pl.when((j >= 0) & (j < chunks))
            def _():
                event(p, j)

        done = r - final

        @pl.when((done >= 0) & (done < chunks))
        def _():
            update(done)

    @pl.loop(0, chunks)
    def _(j):
        own_n1(j).wait_send()
        own_n2(j).wait_send()
        relay_a(j).wait_send()
        relay_b(j).wait_send()

        @pl.when(has_up)
        def _():
            own_up(j).wait_send()

        x_store(j).wait()

    for cycle in range(cycles):
        for p in range(panels):
            f_remote(cycle, p).wait_send()


def local(rhs, factor, inverses):
    count = lax.axis_size("rows")
    cycles, tile, width = rhs.shape
    panels = inverses.shape[0]
    kpart = factor.shape[3]
    chunks = width // LANES
    bf16, f32 = jnp.bfloat16, jnp.float32
    fac = factor.reshape(cycles * tile, panels * kpart)
    dma = lambda n: pltpu.SemaphoreType.DMA((n,))
    return pl.pallas_call(
        functools.partial(kernel, count),
        out_shape=jax.ShapeDtypeStruct(rhs.shape, f32),
        in_specs=[pl.BlockSpec(memory_space=pl.ANY)] * 3,
        out_specs=pl.BlockSpec(memory_space=pl.ANY),
        scratch_shapes=[
            pltpu.VMEM((chunks, panels * tile, LANES), bf16),
            pltpu.VMEM((cycles * tile, panels * tile), bf16),
            pltpu.VMEM((tile, tile), f32),
            pltpu.VMEM((chunks, cycles, tile, LANES), f32),
            dma(cycles * panels), dma(cycles * panels), dma(cycles * panels),
            pltpu.SemaphoreType.DMA, dma(chunks), dma(chunks),
            dma(chunks), dma(chunks), dma(chunks), dma(chunks), dma(chunks),
            dma(chunks), dma(chunks), dma(chunks), dma(chunks), dma(chunks),
        ],
        compiler_params=pltpu.CompilerParams(
            collective_id=0, has_side_effects=True, vmem_limit_bytes=56 << 20
        ),
        name="substitute",
    )(rhs, fac, inverses)


def solution(mesh):
    return jax.shard_map(
        local,
        mesh=mesh,
        in_specs=(P(None, "rows", "rhs"), P(None, "rows", None, "rhs"), P()),
        out_specs=P(None, "rows", "rhs"),
        check_vma=False,
    )
```

```python
import functools

import jax
import jax.numpy as jnp
from jax import lax
from jax.experimental import pallas as pl
from jax.experimental.pallas import tpu as pltpu
from jax.sharding import PartitionSpec as P

LANES = 128
PARTS = 2
SHARE = 10
FIRST = (
    (111366568, 152736309, 148181557, 685019561, 105460297, 415839849, 105682125, 105460317, 307013197, 219780934, 321430683, 325391518, 577582161, 596232348, 460437146, 1073741795, 1073741823),
    (891316800, 891316800, 688417344, 13996230, 90452393, 55143112, 896344614, 642602560, 843756056, 306885144, 10760499, 449652057, 323889562, 443132115, 323826970, 1073741795, 1073741823),
    (285474816, 97026606, 136504385, 17576306, 207981457, 287411098, 154240558, 414819186, 776243416, 414782168, 97030424, 297341531, 425865587, 294444241, 460437363, 1073741795, 1073741823),
    (17043520, 774706241, 633709184, 111518336, 772609088, 772609092, 144344706, 18519690, 349451345, 35869392, 438987354, 892143016, 47461460, 170027546, 725969498, 1073741798, 1073741823),
)
ABOVE = (
    (13897024, 138052149, 245400488, 37389378, 36183169, 507544693, 379654725, 824332507, 420008083, 513835946, 270873883, 69842344, 172956312, 455649371, 458335321, 323823834, 1066252059),
    (136532488, 148144693, 891325768, 292246024, 688196939, 271688406, 64270446, 185553416, 474582344, 282374232, 185342098, 308360238, 186291724, 323611224, 592263314, 342468250, 1066247834),
    (270565376, 841030544, 97027141, 152512083, 414781576, 810297537, 809804317, 270931499, 189195907, 436292506, 155292206, 407997338, 319337330, 711280181, 711267022, 514435278, 1066252059),
    (150995520, 774706824, 439125058, 406853966, 285926097, 648386184, 694525954, 648126678, 45626049, 828945472, 892084965, 483763848, 299212800, 474146443, 292084944, 860702067, 1066874069),
)
X_FIRST = (0x2bede654, 0xfffc99d2, 0x15473ff, 0x81389afe)
Y_FIRST = (0xd41219ab, 0x3662d, 0xfeab8c00, 0x7ec76501)
X_ABOVE = (0x40a0586c, 0x5338849b, 0x10a046b8, 0x7c10c41)
Y_ABOVE = (0x20068100, 0x20a24, 0xef4e2044, 0xf8168004)
U_ABOVE = (0x9f592693, 0xacc57140, 0x119903, 0x2873ba)


def pick(place, values):
    total = jnp.int32(0)
    for i, v in enumerate(values):
        total = total + jnp.where(place == i, jnp.int32(v), jnp.int32(0))
    return total


def signed(mask):
    return mask - (1 << 32) if mask >= 1 << 31 else mask


def split(x):
    high = x.astype(jnp.bfloat16)
    return high, (x - high.astype(jnp.float32)).astype(jnp.bfloat16)


def kernel(count, rhs, fac, inv, out, sent, fbuf, ibuf, ihigh, ilow, xbuf,
           f_in, f_send, f_recv, i_in, x_in, x_out,
           own_recv, a_recv, b_recv, d_recv,
           x_send, y_send, up_send, rx_send, ry_send, ru_send):
    chunks, cycles, tile, lanes = xbuf.shape
    panels = inv.shape[0]
    kpart = fac.shape[1] // panels
    size = tile // PARTS
    planes = count // panels
    bf16, f32 = jnp.bfloat16, jnp.float32

    me = lax.axis_index("rows")
    core = lax.axis_index("rhs")
    z = me // panels
    c = me % panels
    n1 = c + 1 - 2 * (c % 2)
    n2 = (c + 2) % panels
    across = panels - 1 - c
    base = z * panels
    to_core = {"rows": me, "rhs": 1 - core}
    to_n1 = {"rows": base + n1, "rhs": core}
    to_n2 = {"rows": base + n2, "rhs": core}
    to_up = {"rows": jnp.minimum(me + panels, count - 1), "rhs": core}
    to_down = {"rows": jnp.maximum(me - panels, 0), "rhs": core}
    solves = z == 0
    has_up = z < planes - 1
    early = solves & (c == 0)

    def table(first, above, place):
        return jnp.where(solves, pick(place, first), pick(place, above))

    x_mask = table([signed(m) for m in X_FIRST], [signed(m) for m in X_ABOVE], n1)
    y_mask = table([signed(m) for m in Y_FIRST], [signed(m) for m in Y_ABOVE], n2)
    u_mask = jnp.where(has_up, pick(c, [signed(m) for m in U_ABOVE]), 0)

    def bit(mask, k):
        return (jnp.right_shift(mask, k) & 1) == 1

    def x_load(j):
        cols = pl.ds(pl.multiple_of(j * lanes, lanes), lanes)
        return pltpu.make_async_copy(rhs.at[:, :, cols], xbuf.at[j], x_in.at[j])

    def x_store(j):
        cols = pl.ds(pl.multiple_of(j * lanes, lanes), lanes)
        return pltpu.make_async_copy(xbuf.at[j], out.at[:, :, cols], x_out.at[j])

    def i_load():
        return pltpu.make_async_copy(inv.at[c], ibuf, i_in)

    def f_parts(cycle, p, half):
        src = fac.at[pl.ds(cycle * tile, tile), pl.ds(p * kpart, kpart)]
        at = pl.multiple_of(p * 2 * kpart + half * kpart, kpart)
        return src, fbuf.at[pl.ds(cycle * tile, tile), pl.ds(at, kpart)], cycle * panels + p

    def f_local(cycle, p):
        src, dst, at = f_parts(cycle, p, core)
        return pltpu.make_async_copy(src, dst, f_in.at[at])

    def f_remote(cycle, p, half):
        src, dst, at = f_parts(cycle, p, half)
        return pltpu.make_async_remote_copy(src, dst, f_send.at[at], f_recv.at[at], device_id=to_core)

    def hop(p, k, send, recv, to):
        at = pl.multiple_of(p * tile + (k % PARTS) * size, size)
        ref = sent.at[k // PARTS, pl.ds(at, size)]
        return pltpu.make_async_remote_copy(ref, ref, send.at[k], recv.at[k], device_id=to)

    own_x = lambda k: hop(c, k, x_send, a_recv, to_n1)
    own_y = lambda k: hop(c, k, y_send, b_recv, to_n2)
    own_up = lambda k: hop(c, k, up_send, own_recv, to_up)
    relay_x = lambda k: hop(n2, k, rx_send, d_recv, to_n1)
    relay_y = lambda k: hop(n1, k, ry_send, d_recv, to_n2)
    relay_up = lambda k: hop(across, k, ru_send, d_recv, to_up)
    arrive_a = lambda k: hop(n1, k, x_send, a_recv, to_n1)
    arrive_b = lambda k: hop(n2, k, y_send, b_recv, to_n2)
    arrive_d = lambda k: hop(across, k, rx_send, d_recv, to_n1)

    barrier = pltpu.get_barrier_semaphore()
    for to in (to_core, to_n1, to_n2):
        pl.semaphore_signal(barrier, inc=1, device_id=to)

    @pl.when(has_up)
    def _():
        pl.semaphore_signal(barrier, inc=1, device_id=to_up)

    @pl.when(z > 0)
    def _():
        pl.semaphore_signal(barrier, inc=1, device_id=to_down)

    @pl.when(solves)
    def _():
        i_load().start()

    x_load(0).start()
    for cycle in range(cycles):
        for p in range(panels):
            f_local(cycle, p).start()

    @pl.loop(1, chunks)
    def _(j):
        x_load(j).start()

    pl.semaphore_wait(barrier, 3 + jnp.where(has_up, 1, 0) + jnp.where(z > 0, 1, 0))

    for cycle in range(cycles):
        for p in range(panels):
            f_remote(cycle, p, core).start()

    def f_wait(cycle):
        for p in range(panels):
            f_local(cycle, p).wait()
            f_remote(cycle, p, 1 - core).wait_recv()

    @pl.when(solves)
    def _():
        i_load().wait()
        high, low = split(ibuf[...])
        ihigh[...] = high
        ilow[...] = low

    @pl.when(jnp.logical_not(early))
    def _():
        @pl.loop(0, chunks)
        def _(j):
            x_load(j).wait()

    @pl.when(solves & (c > 0))
    def _():
        f_wait(0)

    def correct(p, j):
        rows = slice(p * tile, (p + 1) * tile)
        delta = jnp.dot(fbuf[:tile, rows], sent[j, rows], preferred_element_type=f32)
        xbuf[j, 0] = xbuf[j, 0] - delta

    def solve(p, j):
        if p == 0:
            x_load(j).wait()
        high, low = split(xbuf[j, 0])
        both = jnp.concatenate([high, low], axis=1)
        for r in range(PARTS):
            rows = slice(r * size, (r + 1) * size)
            depth = (r + 1) * size
            wide = jnp.dot(ihigh[rows, :depth], both[:depth], preferred_element_type=f32)
            rest = jnp.dot(ilow[rows, :depth], high[:depth], preferred_element_type=f32)
            solved = rest + wide[:, lanes:] + wide[:, :lanes]
            sent[j, p * tile + r * size:p * tile + (r + 1) * size] = solved.astype(bf16)
            xbuf[j, 0, rows] = solved

    def take(p, k):
        @pl.when(p == c)
        def _():
            @pl.when(solves)
            def _():
                solve(p, k // PARTS)
                own_up(k).start()
                own_up(k + 1).start()

            @pl.when(z > 0)
            def _():
                own_up(k).wait_recv()

                @pl.when(has_up)
                def _():
                    own_up(k).start()

        @pl.when(p == n1)
        def _():
            arrive_a(k).wait_recv()

            @pl.when(bit(y_mask, k))
            def _():
                relay_y(k).start()

        @pl.when(p == n2)
        def _():
            arrive_b(k).wait_recv()

            @pl.when(bit(x_mask, k))
            def _():
                relay_x(k).start()

        @pl.when(p == across)
        def _():
            arrive_d(k).wait_recv()

            @pl.when(bit(u_mask, k))
            def _():
                relay_up(k).start()

        @pl.when(solves & (p < c) & (k % PARTS == PARTS - 1))
        def _():
            correct(p, k // PARTS)

    def update(u):
        @pl.when(u == 0)
        def _():
            f_wait(1)

            @pl.when((z > 0) | (c == 0))
            def _():
                f_wait(0)

        @pl.loop(jnp.where(solves, 1, 0), cycles)
        def _(cycle):
            rows = pl.ds(pl.multiple_of(cycle * tile, tile), tile)
            both = jnp.concatenate([sent[2 * u], sent[2 * u + 1]], axis=1)
            delta = jnp.dot(fbuf[rows, :], both, preferred_element_type=f32)
            xbuf[2 * u, cycle] = xbuf[2 * u, cycle] - delta[:, :lanes]
            xbuf[2 * u + 1, cycle] = xbuf[2 * u + 1, cycle] - delta[:, lanes:]

        x_store(2 * u).start()
        x_store(2 * u + 1).start()

    words = [table([row[w] for row in FIRST], [row[w] for row in ABOVE], c) for w in range(len(FIRST[0]))]

    def step(_, state):
        word, at, xs, ys, us = state
        symbol = word & 7

        for p in range(panels):
            @pl.when(symbol == p)
            def _():
                take(p, at[p])

        @pl.when(symbol == 4)
        def _():
            update(us)

        @pl.when(symbol == 5)
        def _():
            own_x(2 * xs).start()
            own_x(2 * xs + 1).start()

        @pl.when(symbol == 6)
        def _():
            own_y(2 * ys).start()
            own_y(2 * ys + 1).start()

        at = tuple(
            a + jnp.where(symbol == p, jnp.where(solves & (c == p), PARTS, 1), 0) for p, a in enumerate(at)
        )
        xs = xs + jnp.where(symbol == 5, 1, 0)
        ys = ys + jnp.where(symbol == 6, 1, 0)
        us = us + jnp.where(symbol == 4, 1, 0)
        return jnp.right_shift(word, 3), at, xs, ys, us

    def stride(w, state):
        word = pick(w, [0] * 0)
        for i, value in enumerate(words):
            word = word + jnp.where(w == i, value, 0)
        return lax.fori_loop(0, SHARE, step, (word,) + state)[1:]

    zero = jnp.int32(0)
    lax.fori_loop(0, len(words), stride, ((zero,) * panels, zero, zero, zero))

    @pl.loop(0, chunks * PARTS)
    def _(k):
        own_x(k).wait_send()
        own_y(k).wait_send()

        @pl.when(has_up)
        def _():
            own_up(k).wait_send()

        @pl.when(bit(x_mask, k))
        def _():
            relay_x(k).wait_send()

        @pl.when(bit(y_mask, k))
        def _():
            relay_y(k).wait_send()

        @pl.when(bit(u_mask, k))
        def _():
            relay_up(k).wait_send()

    @pl.loop(0, chunks)
    def _(j):
        x_store(j).wait()

    for cycle in range(cycles):
        for p in range(panels):
            f_remote(cycle, p, core).wait_send()


def local(rhs, factor, inverses):
    count = lax.axis_size("rows")
    cycles, tile, width = rhs.shape
    panels = inverses.shape[0]
    kpart = factor.shape[3]
    chunks = width // LANES
    units = chunks * PARTS
    bf16, f32 = jnp.bfloat16, jnp.float32
    fac = factor.reshape(cycles * tile, panels * kpart)
    dma = lambda n: pltpu.SemaphoreType.DMA((n,))
    return pl.pallas_call(
        functools.partial(kernel, count),
        out_shape=jax.ShapeDtypeStruct(rhs.shape, f32),
        in_specs=[pl.BlockSpec(memory_space=pl.ANY)] * 3,
        out_specs=pl.BlockSpec(memory_space=pl.ANY),
        scratch_shapes=[
            pltpu.VMEM((chunks, panels * tile, LANES), bf16),
            pltpu.VMEM((cycles * tile, panels * tile), bf16),
            pltpu.VMEM((tile, tile), f32),
            pltpu.VMEM((tile, tile), bf16),
            pltpu.VMEM((tile, tile), bf16),
            pltpu.VMEM((chunks, cycles, tile, LANES), f32),
            dma(cycles * panels), dma(cycles * panels), dma(cycles * panels),
            pltpu.SemaphoreType.DMA, dma(chunks), dma(chunks),
        ] + [dma(units)] * 10,
        compiler_params=pltpu.CompilerParams(
            collective_id=0, has_side_effects=True, vmem_limit_bytes=56 << 20
        ),
        name="substitute",
    )(rhs, fac, inverses)


def solution(mesh):
    return jax.shard_map(
        local,
        mesh=mesh,
        in_specs=(P(None, "rows", "rhs"), P(None, "rows", None, "rhs"), P()),
        out_specs=P(None, "rows", "rhs"),
        check_vma=False,
    )
```

```python
import functools

import jax
import jax.numpy as jnp
from jax import lax
from jax.experimental import pallas as pl
from jax.experimental.pallas import tpu as pltpu
from jax.sharding import PartitionSpec as P

LANES = 128
PARTS = 2
SHARE = 10
FIRST = (
    (111366568, 152736309, 148181557, 685019561, 105460297, 415839849, 105682125, 105460317, 307013197, 219780934, 321430683, 325391518, 577582161, 596232348, 460437146, 1073741795, 1073741823),
    (891316800, 891316800, 688417344, 13996230, 90452393, 55143112, 896344614, 642602560, 843756056, 306885144, 10760499, 449652057, 323889562, 443132115, 323826970, 1073741795, 1073741823),
    (285474816, 97026606, 136504385, 17576306, 207981457, 287411098, 154240558, 414819186, 776243416, 414782168, 97030424, 297341531, 425865587, 294444241, 460437363, 1073741795, 1073741823),
    (17043520, 774706241, 633709184, 111518336, 772609088, 772609092, 144344706, 18519690, 349451345, 35869392, 438987354, 892143016, 47461460, 170027546, 725969498, 1073741798, 1073741823),
)
ABOVE = (
    (13897024, 138052149, 245400488, 37389378, 36183169, 507544693, 379654725, 824332507, 420008083, 513835946, 270873883, 69842344, 172956312, 455649371, 458335321, 323823834, 1066252059),
    (136532488, 148144693, 891325768, 292246024, 688196939, 271688406, 64270446, 185553416, 474582344, 282374232, 185342098, 308360238, 186291724, 323611224, 592263314, 342468250, 1066247834),
    (270565376, 841030544, 97027141, 152512083, 414781576, 810297537, 809804317, 270931499, 189195907, 436292506, 155292206, 407997338, 319337330, 711280181, 711267022, 514435278, 1066252059),
    (150995520, 774706824, 439125058, 406853966, 285926097, 648386184, 694525954, 648126678, 45626049, 828945472, 892084965, 483763848, 299212800, 474146443, 292084944, 860702067, 1066874069),
)
X_FIRST = (0x2bede654, 0xfffc99d2, 0x15473ff, 0x81389afe)
Y_FIRST = (0xd41219ab, 0x3662d, 0xfeab8c00, 0x7ec76501)
X_ABOVE = (0x40a0586c, 0x5338849b, 0x10a046b8, 0x7c10c41)
Y_ABOVE = (0x20068100, 0x20a24, 0xef4e2044, 0xf8168004)
U_ABOVE = (0x9f592693, 0xacc57140, 0x119903, 0x2873ba)


def pick(place, values):
    total = jnp.int32(0)
    for i, v in enumerate(values):
        total = total + jnp.where(place == i, jnp.int32(v), jnp.int32(0))
    return total


def signed(mask):
    return mask - (1 << 32) if mask >= 1 << 31 else mask


def split(x):
    high = x.astype(jnp.bfloat16)
    return high, (x - high.astype(jnp.float32)).astype(jnp.bfloat16)


def kernel(count, rhs, fac, inv, xbuf, sent, fbuf, ibuf, ihigh, ilow,
           f_in, f_send, f_recv, i_in, x_in,
           own_recv, a_recv, b_recv, d_recv,
           x_send, y_send, up_send, rx_send, ry_send, ru_send):
    chunks, cycles, tile, lanes = xbuf.shape
    panels = inv.shape[0]
    kpart = fac.shape[1] // panels
    size = tile // PARTS
    planes = count // panels
    bf16, f32 = jnp.bfloat16, jnp.float32

    me = lax.axis_index("rows")
    core = lax.axis_index("rhs")
    z = me // panels
    c = me % panels
    n1 = c + 1 - 2 * (c % 2)
    n2 = (c + 2) % panels
    across = panels - 1 - c
    base = z * panels
    to_core = {"rows": me, "rhs": 1 - core}
    to_n1 = {"rows": base + n1, "rhs": core}
    to_n2 = {"rows": base + n2, "rhs": core}
    to_up = {"rows": jnp.minimum(me + panels, count - 1), "rhs": core}
    to_down = {"rows": jnp.maximum(me - panels, 0), "rhs": core}
    solves = z == 0
    has_up = z < planes - 1
    early = solves & (c == 0)

    def table(first, above, place):
        return jnp.where(solves, pick(place, first), pick(place, above))

    x_mask = table([signed(m) for m in X_FIRST], [signed(m) for m in X_ABOVE], n1)
    y_mask = table([signed(m) for m in Y_FIRST], [signed(m) for m in Y_ABOVE], n2)
    u_mask = jnp.where(has_up, pick(c, [signed(m) for m in U_ABOVE]), 0)

    def bit(mask, k):
        return (jnp.right_shift(mask, k) & 1) == 1

    def x_load(j):
        cols = pl.ds(pl.multiple_of(j * lanes, lanes), lanes)
        return pltpu.make_async_copy(rhs.at[:, :, cols], xbuf.at[j], x_in.at[j])

    def i_load():
        return pltpu.make_async_copy(inv.at[c], ibuf, i_in)

    def f_parts(cycle, p, half):
        src = fac.at[pl.ds(cycle * tile, tile), pl.ds(p * kpart, kpart)]
        at = pl.multiple_of(p * 2 * kpart + half * kpart, kpart)
        return src, fbuf.at[pl.ds(cycle * tile, tile), pl.ds(at, kpart)], cycle * panels + p

    def f_local(cycle, p):
        src, dst, at = f_parts(cycle, p, core)
        return pltpu.make_async_copy(src, dst, f_in.at[at])

    def f_remote(cycle, p, half):
        src, dst, at = f_parts(cycle, p, half)
        return pltpu.make_async_remote_copy(src, dst, f_send.at[at], f_recv.at[at], device_id=to_core)

    def hop(p, k, send, recv, to):
        at = pl.multiple_of(p * tile + (k % PARTS) * size, size)
        ref = sent.at[k // PARTS, pl.ds(at, size)]
        return pltpu.make_async_remote_copy(ref, ref, send.at[k], recv.at[k], device_id=to)

    own_x = lambda k: hop(c, k, x_send, a_recv, to_n1)
    own_y = lambda k: hop(c, k, y_send, b_recv, to_n2)
    own_up = lambda k: hop(c, k, up_send, own_recv, to_up)
    relay_x = lambda k: hop(n2, k, rx_send, d_recv, to_n1)
    relay_y = lambda k: hop(n1, k, ry_send, d_recv, to_n2)
    relay_up = lambda k: hop(across, k, ru_send, d_recv, to_up)
    arrive_a = lambda k: hop(n1, k, x_send, a_recv, to_n1)
    arrive_b = lambda k: hop(n2, k, y_send, b_recv, to_n2)
    arrive_d = lambda k: hop(across, k, rx_send, d_recv, to_n1)

    barrier = pltpu.get_barrier_semaphore()
    for to in (to_core, to_n1, to_n2):
        pl.semaphore_signal(barrier, inc=1, device_id=to)

    @pl.when(has_up)
    def _():
        pl.semaphore_signal(barrier, inc=1, device_id=to_up)

    @pl.when(z > 0)
    def _():
        pl.semaphore_signal(barrier, inc=1, device_id=to_down)

    @pl.when(solves)
    def _():
        i_load().start()

    x_load(0).start()
    for cycle in range(cycles):
        for p in range(panels):
            f_local(cycle, p).start()

    @pl.loop(1, chunks)
    def _(j):
        x_load(j).start()

    pl.semaphore_wait(barrier, 3 + jnp.where(has_up, 1, 0) + jnp.where(z > 0, 1, 0))

    for cycle in range(cycles):
        for p in range(panels):
            f_remote(cycle, p, core).start()

    def f_wait(cycle):
        for p in range(panels):
            f_local(cycle, p).wait()
            f_remote(cycle, p, 1 - core).wait_recv()

    @pl.when(solves)
    def _():
        i_load().wait()
        high, low = split(ibuf[...])
        ihigh[...] = high
        ilow[...] = low

    @pl.when(jnp.logical_not(early))
    def _():
        @pl.loop(0, chunks)
        def _(j):
            x_load(j).wait()

    @pl.when(solves & (c > 0))
    def _():
        f_wait(0)

    def correct(p, j):
        rows = slice(p * tile, (p + 1) * tile)
        delta = jnp.dot(fbuf[:tile, rows], sent[j, rows], preferred_element_type=f32)
        xbuf[j, 0] = xbuf[j, 0] - delta

    def solve(p, j):
        if p == 0:
            x_load(j).wait()
        high, low = split(xbuf[j, 0])
        both = jnp.concatenate([high, low], axis=1)
        for r in range(PARTS):
            rows = slice(r * size, (r + 1) * size)
            depth = (r + 1) * size
            wide = jnp.dot(ihigh[rows, :depth], both[:depth], preferred_element_type=f32)
            rest = jnp.dot(ilow[rows, :depth], high[:depth], preferred_element_type=f32)
            solved = rest + wide[:, lanes:] + wide[:, :lanes]
            sent[j, p * tile + r * size:p * tile + (r + 1) * size] = solved.astype(bf16)
            xbuf[j, 0, rows] = solved

    def take(p, k):
        @pl.when(p == c)
        def _():
            @pl.when(solves)
            def _():
                solve(p, k // PARTS)
                own_up(k).start()
                own_up(k + 1).start()

            @pl.when(z > 0)
            def _():
                own_up(k).wait_recv()

                @pl.when(has_up)
                def _():
                    own_up(k).start()

        @pl.when(p == n1)
        def _():
            arrive_a(k).wait_recv()

            @pl.when(bit(y_mask, k))
            def _():
                relay_y(k).start()

        @pl.when(p == n2)
        def _():
            arrive_b(k).wait_recv()

            @pl.when(bit(x_mask, k))
            def _():
                relay_x(k).start()

        @pl.when(p == across)
        def _():
            arrive_d(k).wait_recv()

            @pl.when(bit(u_mask, k))
            def _():
                relay_up(k).start()

        @pl.when(solves & (p < c) & (k % PARTS == PARTS - 1))
        def _():
            correct(p, k // PARTS)

    def update(u):
        @pl.when(u == 0)
        def _():
            f_wait(1)

            @pl.when((z > 0) | (c == 0))
            def _():
                f_wait(0)

        @pl.loop(jnp.where(solves, 1, 0), cycles)
        def _(cycle):
            rows = pl.ds(pl.multiple_of(cycle * tile, tile), tile)
            both = jnp.concatenate([sent[2 * u], sent[2 * u + 1]], axis=1)
            delta = jnp.dot(fbuf[rows, :], both, preferred_element_type=f32)
            xbuf[2 * u, cycle] = xbuf[2 * u, cycle] - delta[:, :lanes]
            xbuf[2 * u + 1, cycle] = xbuf[2 * u + 1, cycle] - delta[:, lanes:]

    words = [table([row[w] for row in FIRST], [row[w] for row in ABOVE], c) for w in range(len(FIRST[0]))]

    def step(_, state):
        word, at, xs, ys, us = state
        symbol = word & 7

        for p in range(panels):
            @pl.when(symbol == p)
            def _():
                take(p, at[p])

        @pl.when(symbol == 4)
        def _():
            update(us)

        @pl.when(symbol == 5)
        def _():
            own_x(2 * xs).start()
            own_x(2 * xs + 1).start()

        @pl.when(symbol == 6)
        def _():
            own_y(2 * ys).start()
            own_y(2 * ys + 1).start()

        at = tuple(
            a + jnp.where(symbol == p, jnp.where(solves & (c == p), PARTS, 1), 0) for p, a in enumerate(at)
        )
        xs = xs + jnp.where(symbol == 5, 1, 0)
        ys = ys + jnp.where(symbol == 6, 1, 0)
        us = us + jnp.where(symbol == 4, 1, 0)
        return jnp.right_shift(word, 3), at, xs, ys, us

    def stride(w, state):
        word = pick(w, [0] * 0)
        for i, value in enumerate(words):
            word = word + jnp.where(w == i, value, 0)
        return lax.fori_loop(0, SHARE, step, (word,) + state)[1:]

    zero = jnp.int32(0)
    lax.fori_loop(0, len(words), stride, ((zero,) * panels, zero, zero, zero))

    @pl.loop(0, chunks * PARTS)
    def _(k):
        own_x(k).wait_send()
        own_y(k).wait_send()

        @pl.when(has_up)
        def _():
            own_up(k).wait_send()

        @pl.when(bit(x_mask, k))
        def _():
            relay_x(k).wait_send()

        @pl.when(bit(y_mask, k))
        def _():
            relay_y(k).wait_send()

        @pl.when(bit(u_mask, k))
        def _():
            relay_up(k).wait_send()

    for cycle in range(cycles):
        for p in range(panels):
            f_remote(cycle, p, core).wait_send()


def place_out(xbuf, out, sems):
    chunks, _, _, lanes = xbuf.shape

    def store(j):
        cols = pl.ds(pl.multiple_of(j * lanes, lanes), lanes)
        return pltpu.make_async_copy(xbuf.at[j], out.at[:, :, cols], sems.at[j])

    @pl.loop(0, chunks)
    def _(j):
        store(j).start()

    @pl.loop(0, chunks)
    def _(j):
        store(j).wait()


def local(rhs, factor, inverses):
    count = lax.axis_size("rows")
    cycles, tile, width = rhs.shape
    panels = inverses.shape[0]
    kpart = factor.shape[3]
    chunks = width // LANES
    units = chunks * PARTS
    bf16, f32 = jnp.bfloat16, jnp.float32
    fac = factor.reshape(cycles * tile, panels * kpart)
    dma = lambda n: pltpu.SemaphoreType.DMA((n,))
    state = pl.pallas_call(
        functools.partial(kernel, count),
        out_shape=pltpu.VMEM((chunks, cycles, tile, LANES), f32),
        in_specs=[pl.BlockSpec(memory_space=pl.ANY)] * 3,
        out_specs=pl.BlockSpec(memory_space=pltpu.VMEM),
        scratch_shapes=[
            pltpu.VMEM((chunks, panels * tile, LANES), bf16),
            pltpu.VMEM((cycles * tile, panels * tile), bf16),
            pltpu.VMEM((tile, tile), f32),
            pltpu.VMEM((tile, tile), bf16),
            pltpu.VMEM((tile, tile), bf16),
            dma(cycles * panels), dma(cycles * panels), dma(cycles * panels),
            pltpu.SemaphoreType.DMA, dma(chunks),
        ] + [dma(units)] * 10,
        compiler_params=pltpu.CompilerParams(
            collective_id=0, has_side_effects=True, vmem_limit_bytes=40 << 20
        ),
        name="substitute",
    )(rhs, fac, inverses)
    return pl.pallas_call(
        place_out,
        out_shape=jax.ShapeDtypeStruct(rhs.shape, f32),
        in_specs=[pl.BlockSpec(memory_space=pltpu.VMEM)],
        out_specs=pl.BlockSpec(memory_space=pl.ANY),
        scratch_shapes=[dma(chunks)],
        compiler_params=pltpu.CompilerParams(vmem_limit_bytes=16 << 20),
        name="place_out",
    )(state)


def solution(mesh):
    return jax.shard_map(
        local,
        mesh=mesh,
        in_specs=(P(None, "rows", "rhs"), P(None, "rows", None, "rhs"), P()),
        out_specs=P(None, "rows", "rhs"),
        check_vma=False,
    )
```

```python
import functools

import jax
import jax.numpy as jnp
from jax import lax
from jax.experimental import pallas as pl
from jax.experimental.pallas import tpu as pltpu
from jax.sharding import PartitionSpec as P

LANES = 128
PARTS = 2
SHARE = 10
FIRST = (
    (111366568, 690180661, 689478214, 306485809, 219730482, 304427673, 689543878, 843889201, 415863912, 289743581, 443328081, 308614302, 577845404, 311277202, 460441307, 1073741795, 1073741823),
    (891316800, 891316800, 891316800, 723544640, 307925190, 81105090, 323697219, 416579866, 891316936, 379859154, 488736531, 327788182, 324089043, 323827859, 443131155, 1073741795, 1073741823),
    (136314880, 809769858, 145171013, 157387650, 143405426, 288218248, 97030702, 140609731, 97026930, 407147291, 187460277, 439143770, 601167477, 893752856, 460437219, 1073741795, 1073741823),
    (17043520, 407179329, 721986101, 856203366, 778376261, 423690308, 36209205, 858270067, 79266901, 5714570, 36330698, 895812979, 47547476, 36334282, 725946795, 1073741798, 1073741823),
)
ABOVE = (
    (13897024, 17256501, 30675061, 352591169, 245896206, 168251472, 174431568, 74403906, 35724610, 40416373, 286372776, 292350481, 342176401, 290559699, 441001179, 457848540, 1066252059),
    (136532488, 148144693, 891325768, 136532488, 315916853, 320509451, 892082328, 276467800, 4595922, 688687017, 306309710, 64259683, 444240579, 309404882, 575485666, 476685971, 1065985746),
    (18874368, 841505922, 776012365, 845230152, 341914181, 407638952, 845222770, 270833861, 273443480, 424415790, 54715092, 177019634, 189108592, 860989298, 153543893, 499992217, 1066252059),
    (136348160, 189010440, 54533466, 438652250, 436493505, 170024144, 97289808, 856265810, 231543013, 3335706, 97322632, 194458714, 2972881, 175184794, 859939187, 778385549, 1066067610),
)
X_FIRST = (0xf77f124, 0xdf7fdd71, 0x1e5eef, 0x820ceafe)
Y_FIRST = (0xf0880edb, 0x2080228e, 0xffe1a110, 0x7df31501)
X_ABOVE = (0x18e64004, 0xee9b4821, 0x88868a1, 0x23043300)
Y_ABOVE = (0x2008289, 0x542, 0xb672120c, 0xdc78cc00)
U_ABOVE = (0xe5193d72, 0x1164b29c, 0x41058552, 0x8300ff)


def pick(place, values):
    total = jnp.int32(0)
    for i, v in enumerate(values):
        total = total + jnp.where(place == i, jnp.int32(v), jnp.int32(0))
    return total


def signed(mask):
    return mask - (1 << 32) if mask >= 1 << 31 else mask


def split(x):
    high = x.astype(jnp.bfloat16)
    return high, (x - high.astype(jnp.float32)).astype(jnp.bfloat16)


def kernel(count, rhs, fac, inv, xbuf, sent, fbuf, fraw, ibuf, ihigh, ilow,
           f_in, f_send, f_recv, i_in, x_in,
           own_recv, a_recv, b_recv, d_recv,
           x_send, y_send, next_send, prev_send, rx_send, ry_send, rn_send, rp_send):
    chunks, cycles, tile, lanes = xbuf.shape
    panels = inv.shape[0]
    kpart = fac.shape[3]
    size = tile // PARTS
    planes = count // panels
    bf16, f32 = jnp.bfloat16, jnp.float32

    me = lax.axis_index("rows")
    core = lax.axis_index("rhs")
    z = me // panels
    c = me % panels
    n1 = c + 1 - 2 * (c % 2)
    n2 = (c + 2) % panels
    across = panels - 1 - c
    base = z * panels
    to_core = {"rows": me, "rhs": 1 - core}
    to_n1 = {"rows": base + n1, "rhs": core}
    to_n2 = {"rows": base + n2, "rhs": core}
    middle = planes // 2
    solves = z == 0
    source = jnp.where(z == middle, 0, jnp.where(z < middle, z + 1, z - 1))
    to_next = ((z == 0) & (planes > 1)) | ((z >= middle) & (z > 0) & (z < planes - 1))
    to_prev = (z <= middle) & (z > 1)
    next_plane = jnp.where(z == 0, middle, jnp.minimum(z + 1, planes - 1))
    at_next = {"rows": next_plane * panels + c, "rhs": core}
    at_prev = {"rows": jnp.maximum(z - 1, 0) * panels + c, "rhs": core}
    at_source = {"rows": source * panels + c, "rhs": core}
    early = solves & (c == 0)

    def table(first, above, place):
        return jnp.where(solves, pick(place, first), pick(place, above))

    x_mask = table([signed(m) for m in X_FIRST], [signed(m) for m in X_ABOVE], n1)
    y_mask = table([signed(m) for m in Y_FIRST], [signed(m) for m in Y_ABOVE], n2)
    u_mask = jnp.where(to_next | to_prev, pick(c, [signed(m) for m in U_ABOVE]), 0)

    def bit(mask, k):
        return (jnp.right_shift(mask, k % 32) & 1) == 1

    def x_load(j):
        cols = pl.ds(pl.multiple_of(j * lanes, lanes), lanes)
        return pltpu.make_async_copy(rhs.at[:, :, cols], xbuf.at[j], x_in.at[j])

    def i_load():
        return pltpu.make_async_copy(inv.at[c], ibuf, i_in)

    def f_load(cycle):
        return pltpu.make_async_copy(fac.at[cycle], fraw.at[cycle], f_in.at[cycle])

    def f_remote(cycle, p, half):
        at = pl.multiple_of(p * 2 * kpart + half * kpart, kpart)
        ref = fbuf.at[pl.ds(cycle * tile, tile), pl.ds(at, kpart)]
        s = cycle * panels + p
        return pltpu.make_async_remote_copy(ref, ref, f_send.at[s], f_recv.at[s], device_id=to_core)

    def f_place(cycle):
        f_load(cycle).wait()
        step = 64

        @pl.loop(0, tile // step)
        def _(i):
            rows = pl.ds(pl.multiple_of(i * step, step), step)
            to = pl.ds(pl.multiple_of(cycle * tile + i * step, step), step)
            block = jnp.transpose(fraw[cycle, rows], (1, 0, 2))
            for p in range(panels):
                at = pl.multiple_of(p * 2 * kpart + core * kpart, kpart)
                fbuf[to, pl.ds(at, kpart)] = block[p]

    def f_share(cycle):
        for p in range(panels):
            f_remote(cycle, p, core).start()

    def hop(p, k, send, recv, to):
        at = pl.multiple_of(p * tile + (k % PARTS) * size, size)
        ref = sent.at[k // PARTS, pl.ds(at, size)]
        return pltpu.make_async_remote_copy(ref, ref, send.at[k], recv.at[k], device_id=to)

    own_x = lambda k: hop(c, k, x_send, a_recv, to_n1)
    own_y = lambda k: hop(c, k, y_send, b_recv, to_n2)
    own_next = lambda k: hop(c, k, next_send, own_recv, at_next)
    own_prev = lambda k: hop(c, k, prev_send, own_recv, at_prev)
    relay_x = lambda k: hop(n2, k, rx_send, d_recv, to_n1)
    relay_y = lambda k: hop(n1, k, ry_send, d_recv, to_n2)
    relay_next = lambda k: hop(across, k, rn_send, d_recv, at_next)
    relay_prev = lambda k: hop(across, k, rp_send, d_recv, at_prev)
    arrive_a = lambda k: hop(n1, k, x_send, a_recv, to_n1)
    arrive_b = lambda k: hop(n2, k, y_send, b_recv, to_n2)
    arrive_d = lambda k: hop(across, k, rx_send, d_recv, to_n1)

    barrier = pltpu.get_barrier_semaphore()
    for to in (to_core, to_n1, to_n2):
        pl.semaphore_signal(barrier, inc=1, device_id=to)

    for on, to in ((to_next, at_next), (to_prev, at_prev), (z > 0, at_source)):
        @pl.when(on)
        def _():
            pl.semaphore_signal(barrier, inc=1, device_id=to)

    @pl.when(solves)
    def _():
        i_load().start()

    x_load(0).start()
    for cycle in range(cycles):
        f_load(cycle).start()

    @pl.loop(1, chunks)
    def _(j):
        x_load(j).start()

    def f_wait(cycle):
        for p in range(panels):
            f_remote(cycle, p, 1 - core).wait_recv()

    @pl.when(solves)
    def _():
        i_load().wait()
        high, low = split(ibuf[...])
        ihigh[...] = high
        ilow[...] = low

    def correct(p, j):
        rows = slice(p * tile, (p + 1) * tile)
        delta = jnp.dot(fbuf[:tile, rows], sent[j, rows], preferred_element_type=f32)
        xbuf[j, 0] = xbuf[j, 0] - delta

    def solve(p, j):
        if p == 0:
            x_load(j).wait()
        high, low = split(xbuf[j, 0])
        both = jnp.concatenate([high, low], axis=1)
        block = tile // 2
        for r in range(2):
            rows = slice(r * block, (r + 1) * block)
            depth = (r + 1) * block
            wide = jnp.dot(ihigh[rows, :depth], both[:depth], preferred_element_type=f32)
            rest = jnp.dot(ilow[rows, :depth], high[:depth], preferred_element_type=f32)
            solved = rest + wide[:, lanes:] + wide[:, :lanes]
            sent[j, p * tile + r * block:p * tile + (r + 1) * block] = solved.astype(bf16)
            xbuf[j, 0, rows] = solved

    @pl.when(early)
    def _():
        solve(0, 0)

    @pl.when(jnp.logical_not(early))
    def _():
        for cycle in range(cycles):
            f_place(cycle)

    words = [table([row[w] for row in FIRST], [row[w] for row in ABOVE], c) for w in range(len(FIRST[0]))]
    pl.semaphore_wait(
        barrier, 3 + jnp.where(to_next, 1, 0) + jnp.where(to_prev, 1, 0) + jnp.where(z > 0, 1, 0)
    )

    @pl.when(jnp.logical_not(early))
    def _():
        for cycle in range(cycles):
            f_share(cycle)

        @pl.loop(0, chunks)
        def _(j):
            x_load(j).wait()

    @pl.when(solves & (c > 0))
    def _():
        f_wait(0)

    def take(p, k):
        @pl.when(p == c)
        def _():
            @pl.when(solves)
            def _():
                if p == 0:
                    @pl.when(k > 0)
                    def _():
                        solve(p, k // PARTS)
                else:
                    solve(p, k // PARTS)

                @pl.when(to_next)
                def _():
                    for i in range(PARTS):
                        own_next(k + i).start()

                if p == 0:
                    @pl.when(k == 3 * PARTS)
                    def _():
                        for cycle in range(cycles):
                            f_place(cycle)
                        for cycle in range(cycles):
                            f_share(cycle)

            @pl.when(z > 0)
            def _():
                own_next(k).wait_recv()

                @pl.when(to_next)
                def _():
                    own_next(k).start()

                @pl.when(to_prev)
                def _():
                    own_prev(k).start()

        @pl.when(p == n1)
        def _():
            arrive_a(k).wait_recv()

            @pl.when(bit(y_mask, k))
            def _():
                relay_y(k).start()

        @pl.when(p == n2)
        def _():
            arrive_b(k).wait_recv()

            @pl.when(bit(x_mask, k))
            def _():
                relay_x(k).start()

        @pl.when(p == across)
        def _():
            arrive_d(k).wait_recv()

            @pl.when(bit(u_mask, k) & to_next)
            def _():
                relay_next(k).start()

            @pl.when(bit(u_mask, k) & to_prev)
            def _():
                relay_prev(k).start()

        @pl.when(solves & (p < c) & (k % PARTS == PARTS - 1))
        def _():
            correct(p, k // PARTS)

    def update(u):
        @pl.when(u == 0)
        def _():
            f_wait(1)

            @pl.when((z > 0) | (c == 0))
            def _():
                f_wait(0)

        @pl.loop(jnp.where(solves, 1, 0), cycles)
        def _(cycle):
            rows = pl.ds(pl.multiple_of(cycle * tile, tile), tile)
            both = jnp.concatenate([sent[2 * u], sent[2 * u + 1]], axis=1)
            delta = jnp.dot(fbuf[rows, :], both, preferred_element_type=f32)
            xbuf[2 * u, cycle] = xbuf[2 * u, cycle] - delta[:, :lanes]
            xbuf[2 * u + 1, cycle] = xbuf[2 * u + 1, cycle] - delta[:, lanes:]

    def step(_, state):
        word, at, xs, ys, us = state
        symbol = word & 7

        for p in range(panels):
            @pl.when(symbol == p)
            def _():
                take(p, at[p])

        @pl.when(symbol == 4)
        def _():
            update(us)

        @pl.when(symbol == 5)
        def _():
            for i in range(PARTS):
                own_x(PARTS * xs + i).start()

        @pl.when(symbol == 6)
        def _():
            for i in range(PARTS):
                own_y(PARTS * ys + i).start()

        at = tuple(
            a + jnp.where(symbol == p, jnp.where(solves & (c == p), PARTS, 1), 0) for p, a in enumerate(at)
        )
        xs = xs + jnp.where(symbol == 5, 1, 0)
        ys = ys + jnp.where(symbol == 6, 1, 0)
        us = us + jnp.where(symbol == 4, 1, 0)
        return jnp.right_shift(word, 3), at, xs, ys, us

    def stride(w, state):
        word = pick(w, [0] * 0)
        for i, value in enumerate(words):
            word = word + jnp.where(w == i, value, 0)
        return lax.fori_loop(0, SHARE, step, (word,) + state)[1:]

    zero = jnp.int32(0)
    lax.fori_loop(0, len(words), stride, ((zero,) * panels, zero, zero, zero))

    @pl.loop(0, chunks * PARTS)
    def _(k):
        own_x(k).wait_send()
        own_y(k).wait_send()

        @pl.when(to_next)
        def _():
            own_next(k).wait_send()

        @pl.when(to_prev)
        def _():
            own_prev(k).wait_send()

        @pl.when(bit(x_mask, k))
        def _():
            relay_x(k).wait_send()

        @pl.when(bit(y_mask, k))
        def _():
            relay_y(k).wait_send()

        @pl.when(bit(u_mask, k) & to_next)
        def _():
            relay_next(k).wait_send()

        @pl.when(bit(u_mask, k) & to_prev)
        def _():
            relay_prev(k).wait_send()

    for cycle in range(cycles):
        for p in range(panels):
            f_remote(cycle, p, core).wait_send()


def place_out(xbuf, out, sems):
    chunks, _, _, lanes = xbuf.shape

    def store(j):
        cols = pl.ds(pl.multiple_of(j * lanes, lanes), lanes)
        return pltpu.make_async_copy(xbuf.at[j], out.at[:, :, cols], sems.at[j])

    @pl.loop(0, chunks)
    def _(j):
        store(j).start()

    @pl.loop(0, chunks)
    def _(j):
        store(j).wait()


def local(rhs, factor, inverses):
    count = lax.axis_size("rows")
    cycles, tile, width = rhs.shape
    panels = inverses.shape[0]
    kpart = factor.shape[3]
    chunks = width // LANES
    units = chunks * PARTS
    bf16, f32 = jnp.bfloat16, jnp.float32
    dma = lambda n: pltpu.SemaphoreType.DMA((n,))
    state = pl.pallas_call(
        functools.partial(kernel, count),
        out_shape=pltpu.VMEM((chunks, cycles, tile, LANES), f32),
        in_specs=[pl.BlockSpec(memory_space=pltpu.HBM)] * 3,
        out_specs=pl.BlockSpec(memory_space=pltpu.VMEM),
        scratch_shapes=[
            pltpu.VMEM((chunks, panels * tile, LANES), bf16),
            pltpu.VMEM((cycles * tile, panels * tile), bf16),
            pltpu.VMEM(factor.shape, bf16),
            pltpu.VMEM((tile, tile), f32),
            pltpu.VMEM((tile, tile), bf16),
            pltpu.VMEM((tile, tile), bf16),
            dma(cycles), dma(cycles * panels), dma(cycles * panels),
            pltpu.SemaphoreType.DMA, dma(chunks),
        ] + [dma(units)] * 12,
        compiler_params=pltpu.CompilerParams(
            collective_id=0, has_side_effects=True, vmem_limit_bytes=55 << 20
        ),
        name="substitute",
    )(rhs, factor, inverses)
    return pl.pallas_call(
        place_out,
        out_shape=jax.ShapeDtypeStruct(rhs.shape, f32),
        in_specs=[pl.BlockSpec(memory_space=pltpu.VMEM)],
        out_specs=pl.BlockSpec(memory_space=pl.ANY),
        scratch_shapes=[dma(chunks)],
        compiler_params=pltpu.CompilerParams(vmem_limit_bytes=16 << 20),
        name="place_out",
    )(state)


def solution(mesh):
    return jax.shard_map(
        local,
        mesh=mesh,
        in_specs=(P(None, "rows", "rhs"), P(None, "rows", None, "rhs"), P()),
        out_specs=P(None, "rows", "rhs"),
        check_vma=False,
    )
```

```python
import functools

import jax
import jax.numpy as jnp
from jax import lax
from jax.experimental import pallas as pl
from jax.experimental.pallas import tpu as pltpu
from jax.sharding import PartitionSpec as P

LANES = 128
PARTS = 2
SHARE = 10
FIRST = (
    (111366568, 690180661, 689478214, 306485809, 219730482, 304427673, 689543878, 843889201, 415863912, 289743581, 443328081, 308614302, 577845404, 311277202, 460441307, 1073741795, 1073741823),
    (891316800, 891316800, 891316800, 723544640, 307925190, 81105090, 323697219, 416579866, 891316936, 379859154, 488736531, 327788182, 324089043, 323827859, 443131155, 1073741795, 1073741823),
    (136314880, 809769858, 145171013, 157387650, 143405426, 288218248, 97030702, 140609731, 97026930, 407147291, 187460277, 439143770, 601167477, 893752856, 460437219, 1073741795, 1073741823),
    (17043520, 407179329, 721986101, 856203366, 778376261, 423690308, 36209205, 858270067, 79266901, 5714570, 36330698, 895812979, 47547476, 36334282, 725946795, 1073741798, 1073741823),
)
ABOVE = (
    (13897024, 17256501, 30675061, 352591169, 245896206, 168251472, 174431568, 74403906, 35724610, 40416373, 286372776, 292350481, 342176401, 290559699, 441001179, 457848540, 1066252059),
    (136532488, 148144693, 891325768, 136532488, 315916853, 320509451, 892082328, 276467800, 4595922, 688687017, 306309710, 64259683, 444240579, 309404882, 575485666, 476685971, 1065985746),
    (18874368, 841505922, 776012365, 845230152, 341914181, 407638952, 845222770, 270833861, 273443480, 424415790, 54715092, 177019634, 189108592, 860989298, 153543893, 499992217, 1066252059),
    (136348160, 189010440, 54533466, 438652250, 436493505, 170024144, 97289808, 856265810, 231543013, 3335706, 97322632, 194458714, 2972881, 175184794, 859939187, 778385549, 1066067610),
)
X_FIRST = (0xf77f124, 0xdf7fdd71, 0x1e5eef, 0x820ceafe)
Y_FIRST = (0xf0880edb, 0x2080228e, 0xffe1a110, 0x7df31501)
X_ABOVE = (0x18e64004, 0xee9b4821, 0x88868a1, 0x23043300)
Y_ABOVE = (0x2008289, 0x542, 0xb672120c, 0xdc78cc00)
U_ABOVE = (0xe5193d72, 0x1164b29c, 0x41058552, 0x8300ff)


def pick(place, values):
    total = jnp.int32(0)
    for i, v in enumerate(values):
        total = total + jnp.where(place == i, jnp.int32(v), jnp.int32(0))
    return total


def signed(mask):
    return mask - (1 << 32) if mask >= 1 << 31 else mask


def split(x):
    high = x.astype(jnp.bfloat16)
    return high, (x - high.astype(jnp.float32)).astype(jnp.bfloat16)


def kernel(count, rhs, fac, inv, xbuf, sent, fbuf, fraw, ibuf, ihigh, ilow,
           f_in, f_send, f_recv, i_in, x_in,
           own_recv, a_recv, b_recv, d_recv,
           x_send, y_send, next_send, prev_send, rx_send, ry_send, rn_send, rp_send):
    chunks, cycles, tile, lanes = xbuf.shape
    panels = inv.shape[0]
    kpart = fac.shape[3]
    size = tile // PARTS
    planes = count // panels
    bf16, f32 = jnp.bfloat16, jnp.float32

    me = lax.axis_index("rows")
    core = lax.axis_index("rhs")
    z = me // panels
    c = me % panels
    n1 = c + 1 - 2 * (c % 2)
    n2 = (c + 2) % panels
    across = panels - 1 - c
    base = z * panels
    to_core = {"rows": me, "rhs": 1 - core}
    to_n1 = {"rows": base + n1, "rhs": core}
    to_n2 = {"rows": base + n2, "rhs": core}
    middle = planes // 2
    solves = z == 0
    source = jnp.where(z == middle, 0, jnp.where(z < middle, z + 1, z - 1))
    to_next = ((z == 0) & (planes > 1)) | ((z >= middle) & (z > 0) & (z < planes - 1))
    to_prev = (z <= middle) & (z > 1)
    next_plane = jnp.where(z == 0, middle, jnp.minimum(z + 1, planes - 1))
    at_next = {"rows": next_plane * panels + c, "rhs": core}
    at_prev = {"rows": jnp.maximum(z - 1, 0) * panels + c, "rhs": core}
    at_source = {"rows": source * panels + c, "rhs": core}
    early = solves & (c == 0)

    def table(first, above, place):
        return jnp.where(solves, pick(place, first), pick(place, above))

    x_mask = table([signed(m) for m in X_FIRST], [signed(m) for m in X_ABOVE], n1)
    y_mask = table([signed(m) for m in Y_FIRST], [signed(m) for m in Y_ABOVE], n2)
    u_mask = jnp.where(to_next | to_prev, pick(c, [signed(m) for m in U_ABOVE]), 0)

    def bit(mask, k):
        return (jnp.right_shift(mask, k % 32) & 1) == 1

    def x_load(j):
        cols = pl.ds(pl.multiple_of(j * lanes, lanes), lanes)
        return pltpu.make_async_copy(rhs.at[:, :, cols], xbuf.at[j], x_in.at[j])

    def i_load():
        return pltpu.make_async_copy(inv.at[c], ibuf, i_in)

    def f_load(cycle):
        return pltpu.make_async_copy(fac.at[cycle], fraw.at[cycle], f_in.at[cycle])

    def f_remote(cycle, p, half):
        at = pl.multiple_of(p * 2 * kpart + half * kpart, kpart)
        ref = fbuf.at[pl.ds(cycle * tile, tile), pl.ds(at, kpart)]
        s = cycle * panels + p
        return pltpu.make_async_remote_copy(ref, ref, f_send.at[s], f_recv.at[s], device_id=to_core)

    def f_place(cycle):
        f_load(cycle).wait()
        step = 64

        @pl.loop(0, tile // step)
        def _(i):
            rows = pl.ds(pl.multiple_of(i * step, step), step)
            to = pl.ds(pl.multiple_of(cycle * tile + i * step, step), step)
            block = jnp.transpose(fraw[cycle, rows], (1, 0, 2))
            for p in range(panels):
                at = pl.multiple_of(p * 2 * kpart + core * kpart, kpart)
                fbuf[to, pl.ds(at, kpart)] = block[p]

    def f_share(cycle):
        for p in range(panels):
            f_remote(cycle, p, core).start()

    def hop(p, k, send, recv, to):
        at = pl.multiple_of(p * tile + (k % PARTS) * size, size)
        ref = sent.at[k // PARTS, pl.ds(at, size)]
        return pltpu.make_async_remote_copy(ref, ref, send.at[k], recv.at[k], device_id=to)

    own_x = lambda k: hop(c, k, x_send, a_recv, to_n1)
    own_y = lambda k: hop(c, k, y_send, b_recv, to_n2)
    own_next = lambda k: hop(c, k, next_send, own_recv, at_next)
    own_prev = lambda k: hop(c, k, prev_send, own_recv, at_prev)
    relay_x = lambda k: hop(n2, k, rx_send, d_recv, to_n1)
    relay_y = lambda k: hop(n1, k, ry_send, d_recv, to_n2)
    relay_next = lambda k: hop(across, k, rn_send, d_recv, at_next)
    relay_prev = lambda k: hop(across, k, rp_send, d_recv, at_prev)
    arrive_a = lambda k: hop(n1, k, x_send, a_recv, to_n1)
    arrive_b = lambda k: hop(n2, k, y_send, b_recv, to_n2)
    arrive_d = lambda k: hop(across, k, rx_send, d_recv, to_n1)

    barrier = pltpu.get_barrier_semaphore()
    for to in (to_core, to_n1, to_n2):
        pl.semaphore_signal(barrier, inc=1, device_id=to)

    for on, to in ((to_next, at_next), (to_prev, at_prev), (z > 0, at_source)):
        @pl.when(on)
        def _():
            pl.semaphore_signal(barrier, inc=1, device_id=to)

    @pl.when(solves)
    def _():
        i_load().start()

    x_load(0).start()
    for cycle in range(cycles):
        f_load(cycle).start()

    @pl.loop(1, chunks)
    def _(j):
        x_load(j).start()

    def f_wait(cycle):
        for p in range(panels):
            f_remote(cycle, p, 1 - core).wait_recv()

    @pl.when(solves)
    def _():
        i_load().wait()
        high, low = split(ibuf[...])
        ihigh[...] = high
        ilow[...] = low

    def correct(p, j):
        rows = slice(p * tile, (p + 1) * tile)
        delta = jnp.dot(fbuf[:tile, rows], sent[j, rows], preferred_element_type=f32)
        xbuf[j, 0] = xbuf[j, 0] - delta

    def solve(p, j):
        if p == 0:
            x_load(j).wait()
        high, low = split(xbuf[j, 0])
        both = jnp.concatenate([high, low], axis=1)
        block = tile // 2
        for r in range(2):
            rows = slice(r * block, (r + 1) * block)
            depth = (r + 1) * block
            wide = jnp.dot(ihigh[rows, :depth], both[:depth], preferred_element_type=f32)
            rest = jnp.dot(ilow[rows, :depth], high[:depth], preferred_element_type=f32)
            solved = rest + wide[:, lanes:] + wide[:, :lanes]
            sent[j, p * tile + r * block:p * tile + (r + 1) * block] = solved.astype(bf16)
            xbuf[j, 0, rows] = solved

    @pl.when(early)
    def _():
        solve(0, 0)

    @pl.when(jnp.logical_not(early))
    def _():
        for cycle in range(cycles):
            f_place(cycle)

    words = [table([row[w] for row in FIRST], [row[w] for row in ABOVE], c) for w in range(len(FIRST[0]))]
    pl.semaphore_wait(
        barrier, 3 + jnp.where(to_next, 1, 0) + jnp.where(to_prev, 1, 0) + jnp.where(z > 0, 1, 0)
    )

    @pl.when(jnp.logical_not(early))
    def _():
        for cycle in range(cycles):
            f_share(cycle)

        @pl.loop(0, chunks)
        def _(j):
            x_load(j).wait()

    @pl.when(solves & (c > 0))
    def _():
        f_wait(0)

    def take(p, k):
        @pl.when(p == c)
        def _():
            @pl.when(solves)
            def _():
                if p == 0:
                    @pl.when(k > 0)
                    def _():
                        solve(p, k // PARTS)
                else:
                    solve(p, k // PARTS)

                @pl.when(to_next)
                def _():
                    for i in range(PARTS):
                        own_next(k + i).start()

                if p == 0:
                    @pl.when(k == 3 * PARTS)
                    def _():
                        for cycle in range(cycles):
                            f_place(cycle)
                        for cycle in range(cycles):
                            f_share(cycle)

            @pl.when(z > 0)
            def _():
                own_next(k).wait_recv()

                @pl.when(to_next)
                def _():
                    own_next(k).start()

                @pl.when(to_prev)
                def _():
                    own_prev(k).start()

        @pl.when(p == n1)
        def _():
            arrive_a(k).wait_recv()

            @pl.when(bit(y_mask, k))
            def _():
                relay_y(k).start()

        @pl.when(p == n2)
        def _():
            arrive_b(k).wait_recv()

            @pl.when(bit(x_mask, k))
            def _():
                relay_x(k).start()

        @pl.when(p == across)
        def _():
            arrive_d(k).wait_recv()

            @pl.when(bit(u_mask, k) & to_next)
            def _():
                relay_next(k).start()

            @pl.when(bit(u_mask, k) & to_prev)
            def _():
                relay_prev(k).start()

        @pl.when(solves & (p < c) & (k % PARTS == PARTS - 1))
        def _():
            correct(p, k // PARTS)

    def update(u):
        @pl.when(u == 0)
        def _():
            f_wait(1)

            @pl.when((z > 0) | (c == 0))
            def _():
                f_wait(0)

        @pl.loop(jnp.where(solves, 1, 0), cycles)
        def _(cycle):
            rows = pl.ds(pl.multiple_of(cycle * tile, tile), tile)
            both = jnp.concatenate([sent[2 * u], sent[2 * u + 1]], axis=1)
            delta = jnp.dot(fbuf[rows, :], both, preferred_element_type=f32)
            xbuf[2 * u, cycle] = xbuf[2 * u, cycle] - delta[:, :lanes]
            xbuf[2 * u + 1, cycle] = xbuf[2 * u + 1, cycle] - delta[:, lanes:]

    def step(_, state):
        word, at, xs, ys, us = state
        symbol = word & 7

        for p in range(panels):
            @pl.when(symbol == p)
            def _():
                take(p, at[p])

        @pl.when((symbol == 4) & (us < chunks // 2 - 1))
        def _():
            update(us)

        @pl.when(symbol == 5)
        def _():
            for i in range(PARTS):
                own_x(PARTS * xs + i).start()

        @pl.when(symbol == 6)
        def _():
            for i in range(PARTS):
                own_y(PARTS * ys + i).start()

        at = tuple(
            a + jnp.where(symbol == p, jnp.where(solves & (c == p), PARTS, 1), 0) for p, a in enumerate(at)
        )
        xs = xs + jnp.where(symbol == 5, 1, 0)
        ys = ys + jnp.where(symbol == 6, 1, 0)
        us = us + jnp.where(symbol == 4, 1, 0)
        return jnp.right_shift(word, 3), at, xs, ys, us

    def stride(w, state):
        word = pick(w, [0] * 0)
        for i, value in enumerate(words):
            word = word + jnp.where(w == i, value, 0)
        return lax.fori_loop(0, SHARE, step, (word,) + state)[1:]

    zero = jnp.int32(0)
    lax.fori_loop(0, len(words), stride, ((zero,) * panels, zero, zero, zero))

    @pl.loop(0, chunks * PARTS)
    def _(k):
        own_x(k).wait_send()
        own_y(k).wait_send()

        @pl.when(to_next)
        def _():
            own_next(k).wait_send()

        @pl.when(to_prev)
        def _():
            own_prev(k).wait_send()

        @pl.when(bit(x_mask, k))
        def _():
            relay_x(k).wait_send()

        @pl.when(bit(y_mask, k))
        def _():
            relay_y(k).wait_send()

        @pl.when(bit(u_mask, k) & to_next)
        def _():
            relay_next(k).wait_send()

        @pl.when(bit(u_mask, k) & to_prev)
        def _():
            relay_prev(k).wait_send()

    for cycle in range(cycles):
        for p in range(panels):
            f_remote(cycle, p, core).wait_send()


def finish(panels, xbuf, sent, fbuf, out, last, sems):
    chunks, cycles, tile, lanes = xbuf.shape
    first = chunks - 2
    solves = lax.axis_index("rows") < panels

    def store(j, ref):
        cols = pl.ds(pl.multiple_of(j * lanes, lanes), lanes)
        return pltpu.make_async_copy(ref, out.at[:, :, cols], sems.at[j])

    @pl.loop(0, first)
    def _(j):
        store(j, xbuf.at[j]).start()

    @pl.when(solves)
    def _():
        last[:, 0] = xbuf[first:, 0]

    both = jnp.concatenate([sent[first], sent[first + 1]], axis=1)

    @pl.loop(jnp.where(solves, 1, 0), cycles)
    def _(cycle):
        rows = pl.ds(pl.multiple_of(cycle * tile, tile), tile)
        delta = jnp.dot(fbuf[rows, :], both, preferred_element_type=jnp.float32)
        last[0, cycle] = xbuf[first, cycle] - delta[:, :lanes]
        last[1, cycle] = xbuf[first + 1, cycle] - delta[:, lanes:]

    for i in range(2):
        store(first + i, last.at[i]).start()

    @pl.loop(0, chunks)
    def _(j):
        store(j, xbuf.at[j]).wait()


def local(rhs, factor, inverses):
    count = lax.axis_size("rows")
    cycles, tile, width = rhs.shape
    panels = inverses.shape[0]
    kpart = factor.shape[3]
    chunks = width // LANES
    units = chunks * PARTS
    bf16, f32 = jnp.bfloat16, jnp.float32
    dma = lambda n: pltpu.SemaphoreType.DMA((n,))
    vmem = pl.BlockSpec(memory_space=pltpu.VMEM)
    state = pl.pallas_call(
        functools.partial(kernel, count),
        out_shape=(
            pltpu.VMEM((chunks, cycles, tile, LANES), f32),
            pltpu.VMEM((chunks, panels * tile, LANES), bf16),
            pltpu.VMEM((cycles * tile, panels * tile), bf16),
        ),
        in_specs=[pl.BlockSpec(memory_space=pltpu.HBM)] * 3,
        out_specs=(vmem, vmem, vmem),
        scratch_shapes=[
            pltpu.VMEM(factor.shape, bf16),
            pltpu.VMEM((tile, tile), f32),
            pltpu.VMEM((tile, tile), bf16),
            pltpu.VMEM((tile, tile), bf16),
            dma(cycles), dma(cycles * panels), dma(cycles * panels),
            pltpu.SemaphoreType.DMA, dma(chunks),
        ] + [dma(units)] * 12,
        compiler_params=pltpu.CompilerParams(
            collective_id=0, has_side_effects=True, vmem_limit_bytes=43 << 20
        ),
        name="substitute",
    )(rhs, factor, inverses)
    return pl.pallas_call(
        functools.partial(finish, panels),
        out_shape=jax.ShapeDtypeStruct(rhs.shape, f32),
        in_specs=[vmem] * 3,
        out_specs=pl.BlockSpec(memory_space=pl.ANY),
        scratch_shapes=[pltpu.VMEM((2, cycles, tile, LANES), f32), dma(chunks)],
        compiler_params=pltpu.CompilerParams(vmem_limit_bytes=16 << 20),
        name="finish",
    )(*state)


def solution(mesh):
    return jax.shard_map(
        local,
        mesh=mesh,
        in_specs=(P(None, "rows", "rhs"), P(None, "rows", None, "rhs"), P()),
        out_specs=P(None, "rows", "rhs"),
        check_vma=False,
    )
```

```python
import functools

import jax
import jax.numpy as jnp
from jax import lax
from jax.experimental import pallas as pl
from jax.experimental.pallas import tpu as pltpu
from jax.sharding import PartitionSpec as P

LANES = 128
PARTS = 2
SHARE = 10
FIRST = (
    (111366568, 152621109, 152621453, 178594189, 136741718, 105489006, 463672147, 154412425, 437818515, 826594450, 423182930, 309184147, 325960858, 460211931, 594396315, 1073741795, 1073741823),
    (891316800, 891316800, 891507200, 138504768, 11306542, 421179507, 414746501, 407735176, 319399281, 459926082, 460184640, 308913947, 342733979, 340337812, 306783508, 1073741796, 1073741823),
    (134479872, 839130000, 144908813, 410313792, 438668177, 833130924, 285490065, 35757277, 271353768, 893766749, 188240968, 288122410, 288098205, 594425589, 477214428, 1073741795, 1073741823),
    (289706568, 45655553, 169102537, 172004250, 2835800, 173302297, 178397747, 353898705, 56170696, 408235085, 105219488, 306655338, 402742464, 45142421, 768410931, 1073741797, 1073741823),
)
ABOVE = (
    (13896576, 673402933, 19091526, 178524557, 675834374, 51990658, 850067701, 306297728, 170449992, 287650507, 405411464, 442805482, 421860451, 457513106, 439203043, 474846434, 1066252059),
    (148151625, 134244928, 103025705, 688149005, 405602480, 44374920, 406106312, 86087593, 52638233, 13542099, 307600534, 55518297, 374712961, 575354083, 340731099, 577357539, 1065985299),
    (20971520, 35709265, 365498738, 845197384, 380436613, 499234072, 347668506, 269323138, 776524186, 348427482, 556634205, 319294346, 342799241, 189486801, 866690931, 159683291, 1065726556),
    (17076224, 17604680, 424436570, 37863598, 816656755, 188748386, 38547883, 438420806, 52506966, 688669934, 432330398, 422652826, 107832665, 365797461, 22647371, 711304514, 1065697958),
)
X_FIRST = (0xffde842a, 0xf44c0150, 0x560b52ff, 0x80058805)
Y_FIRST = (0x216095, 0x28a3, 0xa9f4ad00, 0x74021000)
X_ABOVE = (0x28f58fa2, 0xefff6e08, 0x40e24a, 0x148546be)
Y_ABOVE = (0x14023045, 0x10009084, 0xbb3e0531, 0x6b7ab940)
U_ABOVE = (0xc3084018, 0x173, 0x44811884, 0x80000001)
D_FIRST = (0x1b40, 0xbb3d60c, 0x0, 0xbf867fa)


def pick(place, values):
    total = jnp.int32(0)
    for i, v in enumerate(values):
        total = total + jnp.where(place == i, jnp.int32(v), jnp.int32(0))
    return total


def signed(mask):
    return mask - (1 << 32) if mask >= 1 << 31 else mask


def split(x):
    high = x.astype(jnp.bfloat16)
    return high, (x - high.astype(jnp.float32)).astype(jnp.bfloat16)


def kernel(count, rhs, fac, inv, xbuf, sent, fbuf, fraw, ibuf, ihigh, ilow,
           f_in, f_send, f_recv, i_in, x_in,
           own_recv, a_recv, b_recv, d_recv,
           x_send, y_send, next_send, prev_send, rx_send, ry_send, rn_send, rp_send, rd_send):
    chunks, cycles, tile, lanes = xbuf.shape
    panels = inv.shape[0]
    kpart = fac.shape[3]
    size = tile // PARTS
    planes = count // panels
    bf16, f32 = jnp.bfloat16, jnp.float32

    me = lax.axis_index("rows")
    core = lax.axis_index("rhs")
    z = me // panels
    c = me % panels
    n1 = c + 1 - 2 * (c % 2)
    n2 = (c + 2) % panels
    across = panels - 1 - c
    base = z * panels
    to_core = {"rows": me, "rhs": 1 - core}
    to_n1 = {"rows": base + n1, "rhs": core}
    to_n2 = {"rows": base + n2, "rhs": core}
    middle = planes // 2
    solves = z == 0
    source = jnp.where(z == middle, 0, jnp.where(z < middle, z + 1, z - 1))
    to_next = ((z == 0) & (planes > 1)) | ((z >= middle) & (z > 0) & (z < planes - 1))
    to_prev = (z <= middle) & (z > 1)
    next_plane = jnp.where(z == 0, middle, jnp.minimum(z + 1, planes - 1))
    at_next = {"rows": next_plane * panels + c, "rhs": core}
    at_prev = {"rows": jnp.maximum(z - 1, 0) * panels + c, "rhs": core}
    at_source = {"rows": source * panels + c, "rhs": core}
    early = solves & (c == 0)

    at_bottom = {"rows": c, "rhs": core}
    at_first = {"rows": jnp.where(planes > 1, panels, 0) + c, "rhs": core}

    def table(first, above, place):
        return jnp.where(solves, pick(place, first), pick(place, above))

    x_mask = table([signed(m) for m in X_FIRST], [signed(m) for m in X_ABOVE], n1)
    y_mask = table([signed(m) for m in Y_FIRST], [signed(m) for m in Y_ABOVE], n2)
    d_mask = jnp.where(z == 1, pick(c, [signed(m) for m in D_FIRST]), 0)
    u_mask = jnp.where(to_next | to_prev, pick(c, [signed(m) for m in U_ABOVE]), 0)

    def bit(mask, k):
        return (jnp.right_shift(mask, k % 32) & 1) == 1

    def x_load(j):
        cols = pl.ds(pl.multiple_of(j * lanes, lanes), lanes)
        return pltpu.make_async_copy(rhs.at[:, :, cols], xbuf.at[j], x_in.at[j])

    def i_load():
        return pltpu.make_async_copy(inv.at[c], ibuf, i_in)

    def f_load(cycle):
        return pltpu.make_async_copy(fac.at[cycle], fraw.at[cycle], f_in.at[cycle])

    def f_remote(cycle, p, half):
        at = pl.multiple_of(p * 2 * kpart + half * kpart, kpart)
        ref = fbuf.at[pl.ds(cycle * tile, tile), pl.ds(at, kpart)]
        s = cycle * panels + p
        return pltpu.make_async_remote_copy(ref, ref, f_send.at[s], f_recv.at[s], device_id=to_core)

    def f_place(cycle):
        f_load(cycle).wait()
        step = 64

        @pl.loop(0, tile // step)
        def _(i):
            rows = pl.ds(pl.multiple_of(i * step, step), step)
            to = pl.ds(pl.multiple_of(cycle * tile + i * step, step), step)
            block = jnp.transpose(fraw[cycle, rows], (1, 0, 2))
            for p in range(panels):
                at = pl.multiple_of(p * 2 * kpart + core * kpart, kpart)
                fbuf[to, pl.ds(at, kpart)] = block[p]

    def f_share(cycle):
        for p in range(panels):
            f_remote(cycle, p, core).start()

    def hop(p, k, send, recv, to):
        at = pl.multiple_of(p * tile + (k % PARTS) * size, size)
        ref = sent.at[k // PARTS, pl.ds(at, size)]
        return pltpu.make_async_remote_copy(ref, ref, send.at[k], recv.at[k], device_id=to)

    own_x = lambda k: hop(c, k, x_send, a_recv, to_n1)
    own_y = lambda k: hop(c, k, y_send, b_recv, to_n2)
    own_next = lambda k: hop(c, k, next_send, own_recv, at_next)
    own_prev = lambda k: hop(c, k, prev_send, own_recv, at_prev)
    relay_x = lambda k: hop(n2, k, rx_send, d_recv, to_n1)
    relay_y = lambda k: hop(n1, k, ry_send, d_recv, to_n2)
    relay_next = lambda k: hop(across, k, rn_send, d_recv, at_next)
    relay_down = lambda k: hop(across, k, rd_send, d_recv, at_bottom)
    relay_prev = lambda k: hop(across, k, rp_send, d_recv, at_prev)
    arrive_a = lambda k: hop(n1, k, x_send, a_recv, to_n1)
    arrive_b = lambda k: hop(n2, k, y_send, b_recv, to_n2)
    arrive_d = lambda k: hop(across, k, rx_send, d_recv, to_n1)

    barrier = pltpu.get_barrier_semaphore()
    for to in (to_core, to_n1, to_n2):
        pl.semaphore_signal(barrier, inc=1, device_id=to)

    apart = middle > 1
    for on, to in (
        (to_next, at_next), (to_prev, at_prev), (z > 0, at_source),
        (solves & apart, at_first), ((z == 1) & apart, at_bottom),
    ):
        @pl.when(on)
        def _():
            pl.semaphore_signal(barrier, inc=1, device_id=to)

    @pl.when(solves)
    def _():
        i_load().start()

    x_load(0).start()

    def load_rest():
        for cycle in range(cycles):
            f_load(cycle).start()

        @pl.loop(1, chunks)
        def _(j):
            x_load(j).start()

    @pl.when(jnp.logical_not(early))
    def _():
        load_rest()

    def f_wait(cycle):
        for p in range(panels):
            f_remote(cycle, p, 1 - core).wait_recv()

    @pl.when(solves)
    def _():
        i_load().wait()
        high, low = split(ibuf[...])
        ihigh[...] = high
        ilow[...] = low

    def correct(p, j):
        rows = slice(p * tile, (p + 1) * tile)
        delta = jnp.dot(fbuf[:tile, rows], sent[j, rows], preferred_element_type=f32)
        xbuf[j, 0] = xbuf[j, 0] - delta

    def solve(p, j):
        if p == 0:
            x_load(j).wait()
        high, low = split(xbuf[j, 0])
        both = jnp.concatenate([high, low], axis=1)
        block = tile // 2
        for r in range(2):
            rows = slice(r * block, (r + 1) * block)
            depth = (r + 1) * block
            wide = jnp.dot(ihigh[rows, :depth], both[:depth], preferred_element_type=f32)
            rest = jnp.dot(ilow[rows, :depth], high[:depth], preferred_element_type=f32)
            solved = rest + wide[:, lanes:] + wide[:, :lanes]
            sent[j, p * tile + r * block:p * tile + (r + 1) * block] = solved.astype(bf16)
            xbuf[j, 0, rows] = solved

    @pl.when(early)
    def _():
        solve(0, 0)
        load_rest()

    @pl.when(jnp.logical_not(early))
    def _():
        for cycle in range(cycles):
            f_place(cycle)

    words = [table([row[w] for row in FIRST], [row[w] for row in ABOVE], c) for w in range(len(FIRST[0]))]
    pl.semaphore_wait(
        barrier,
        3 + jnp.where(to_next, 1, 0) + jnp.where(to_prev, 1, 0) + jnp.where(z > 0, 1, 0)
        + jnp.where((z < 2) & apart, 1, 0),
    )

    @pl.when(jnp.logical_not(early))
    def _():
        for cycle in range(cycles):
            f_share(cycle)

        @pl.loop(0, chunks)
        def _(j):
            x_load(j).wait()

    @pl.when(solves & (c > 0))
    def _():
        f_wait(0)

    def take(p, k):
        @pl.when(p == c)
        def _():
            @pl.when(solves)
            def _():
                if p == 0:
                    @pl.when(k > 0)
                    def _():
                        solve(p, k // PARTS)
                else:
                    solve(p, k // PARTS)

                @pl.when(to_next)
                def _():
                    for i in range(PARTS):
                        own_next(k + i).start()

                if p == 0:
                    @pl.when(k == 3 * PARTS)
                    def _():
                        for cycle in range(cycles):
                            f_place(cycle)
                        for cycle in range(cycles):
                            f_share(cycle)

            @pl.when(z > 0)
            def _():
                own_next(k).wait_recv()

                @pl.when(to_next)
                def _():
                    own_next(k).start()

                @pl.when(to_prev)
                def _():
                    own_prev(k).start()

        @pl.when(p == n1)
        def _():
            arrive_a(k).wait_recv()

            @pl.when(bit(y_mask, k))
            def _():
                relay_y(k).start()

        @pl.when(p == n2)
        def _():
            arrive_b(k).wait_recv()

            @pl.when(bit(x_mask, k))
            def _():
                relay_x(k).start()

        @pl.when(p == across)
        def _():
            arrive_d(k).wait_recv()

            @pl.when(bit(u_mask, k) & to_next)
            def _():
                relay_next(k).start()

            @pl.when(bit(u_mask, k) & to_prev)
            def _():
                relay_prev(k).start()

            @pl.when(bit(d_mask, k))
            def _():
                relay_down(k).start()

        @pl.when(solves & (p < c) & (k % PARTS == PARTS - 1))
        def _():
            correct(p, k // PARTS)

    def update(u):
        @pl.when(u == 0)
        def _():
            f_wait(1)

            @pl.when((z > 0) | (c == 0))
            def _():
                f_wait(0)

        @pl.loop(jnp.where(solves, 1, 0), cycles)
        def _(cycle):
            rows = pl.ds(pl.multiple_of(cycle * tile, tile), tile)
            both = jnp.concatenate([sent[2 * u], sent[2 * u + 1]], axis=1)
            delta = jnp.dot(fbuf[rows, :], both, preferred_element_type=f32)
            xbuf[2 * u, cycle] = xbuf[2 * u, cycle] - delta[:, :lanes]
            xbuf[2 * u + 1, cycle] = xbuf[2 * u + 1, cycle] - delta[:, lanes:]

    def step(_, state):
        word, at, xs, ys, us = state
        symbol = word & 7

        for p in range(panels):
            @pl.when(symbol == p)
            def _():
                take(p, at[p])

        @pl.when((symbol == 4) & (us < chunks // 2 - 1))
        def _():
            update(us)

        @pl.when(symbol == 5)
        def _():
            for i in range(PARTS):
                own_x(PARTS * xs + i).start()

        @pl.when(symbol == 6)
        def _():
            for i in range(PARTS):
                own_y(PARTS * ys + i).start()

        at = tuple(
            a + jnp.where(symbol == p, jnp.where(solves & (c == p), PARTS, 1), 0) for p, a in enumerate(at)
        )
        xs = xs + jnp.where(symbol == 5, 1, 0)
        ys = ys + jnp.where(symbol == 6, 1, 0)
        us = us + jnp.where(symbol == 4, 1, 0)
        return jnp.right_shift(word, 3), at, xs, ys, us

    def stride(w, state):
        word = pick(w, [0] * 0)
        for i, value in enumerate(words):
            word = word + jnp.where(w == i, value, 0)
        return lax.fori_loop(0, SHARE, step, (word,) + state)[1:]

    zero = jnp.int32(0)
    lax.fori_loop(0, len(words), stride, ((zero,) * panels, zero, zero, zero))

    @pl.loop(0, chunks * PARTS)
    def _(k):
        own_x(k).wait_send()
        own_y(k).wait_send()

        @pl.when(to_next)
        def _():
            own_next(k).wait_send()

        @pl.when(to_prev)
        def _():
            own_prev(k).wait_send()

        @pl.when(bit(x_mask, k))
        def _():
            relay_x(k).wait_send()

        @pl.when(bit(y_mask, k))
        def _():
            relay_y(k).wait_send()

        @pl.when(bit(u_mask, k) & to_next)
        def _():
            relay_next(k).wait_send()

        @pl.when(bit(u_mask, k) & to_prev)
        def _():
            relay_prev(k).wait_send()

        @pl.when(bit(d_mask, k))
        def _():
            relay_down(k).wait_send()

    for cycle in range(cycles):
        for p in range(panels):
            f_remote(cycle, p, core).wait_send()


def finish(panels, xbuf, sent, fbuf, out, last, sems):
    chunks, cycles, tile, lanes = xbuf.shape
    first = chunks - 2
    solves = lax.axis_index("rows") < panels

    def store(j, ref):
        cols = pl.ds(pl.multiple_of(j * lanes, lanes), lanes)
        return pltpu.make_async_copy(ref, out.at[:, :, cols], sems.at[j])

    @pl.loop(0, first)
    def _(j):
        store(j, xbuf.at[j]).start()

    @pl.when(solves)
    def _():
        last[:, 0] = xbuf[first:, 0]

    both = jnp.concatenate([sent[first], sent[first + 1]], axis=1)

    @pl.loop(jnp.where(solves, 1, 0), cycles)
    def _(cycle):
        rows = pl.ds(pl.multiple_of(cycle * tile, tile), tile)
        delta = jnp.dot(fbuf[rows, :], both, preferred_element_type=jnp.float32)
        last[0, cycle] = xbuf[first, cycle] - delta[:, :lanes]
        last[1, cycle] = xbuf[first + 1, cycle] - delta[:, lanes:]

    for i in range(2):
        store(first + i, last.at[i]).start()

    @pl.loop(0, chunks)
    def _(j):
        store(j, xbuf.at[j]).wait()


def local(rhs, factor, inverses):
    count = lax.axis_size("rows")
    cycles, tile, width = rhs.shape
    panels = inverses.shape[0]
    kpart = factor.shape[3]
    chunks = width // LANES
    units = chunks * PARTS
    bf16, f32 = jnp.bfloat16, jnp.float32
    dma = lambda n: pltpu.SemaphoreType.DMA((n,))
    vmem = pl.BlockSpec(memory_space=pltpu.VMEM)
    state = pl.pallas_call(
        functools.partial(kernel, count),
        out_shape=(
            pltpu.VMEM((chunks, cycles, tile, LANES), f32),
            pltpu.VMEM((chunks, panels * tile, LANES), bf16),
            pltpu.VMEM((cycles * tile, panels * tile), bf16),
        ),
        in_specs=[pl.BlockSpec(memory_space=pltpu.HBM)] * 3,
        out_specs=(vmem, vmem, vmem),
        scratch_shapes=[
            pltpu.VMEM(factor.shape, bf16),
            pltpu.VMEM((tile, tile), f32),
            pltpu.VMEM((tile, tile), bf16),
            pltpu.VMEM((tile, tile), bf16),
            dma(cycles), dma(cycles * panels), dma(cycles * panels),
            pltpu.SemaphoreType.DMA, dma(chunks),
        ] + [dma(units)] * 13,
        compiler_params=pltpu.CompilerParams(
            collective_id=0, has_side_effects=True, vmem_limit_bytes=43 << 20
        ),
        name="substitute",
    )(rhs, factor, inverses)
    return pl.pallas_call(
        functools.partial(finish, panels),
        out_shape=jax.ShapeDtypeStruct(rhs.shape, f32),
        in_specs=[vmem] * 3,
        out_specs=pl.BlockSpec(memory_space=pl.ANY),
        scratch_shapes=[pltpu.VMEM((2, cycles, tile, LANES), f32), dma(chunks)],
        compiler_params=pltpu.CompilerParams(vmem_limit_bytes=16 << 20),
        name="finish",
    )(*state)


def solution(mesh):
    return jax.shard_map(
        local,
        mesh=mesh,
        in_specs=(P(None, "rows", "rhs"), P(None, "rows", None, "rhs"), P()),
        out_specs=P(None, "rows", "rhs"),
        check_vma=False,
    )
```

```python
import functools

import jax
import jax.numpy as jnp
from jax import lax
from jax.experimental import pallas as pl
from jax.experimental.pallas import tpu as pltpu
from jax.sharding import PartitionSpec as P

LANES = 128
PARTS = 2
SHARE = 10
FIRST = (
    (111366568, 152621109, 152621453, 178594189, 136741718, 105489006, 463672147, 154412425, 437818515, 826594450, 423182930, 309184147, 325960858, 460211931, 594396315, 1073741795, 1073741823),
    (891316800, 891316800, 891507200, 138504768, 11306542, 421179507, 414746501, 407735176, 319399281, 459926082, 460184640, 308913947, 342733979, 340337812, 306783508, 1073741796, 1073741823),
    (134479872, 839130000, 144908813, 410313792, 438668177, 833130924, 285490065, 35757277, 271353768, 893766749, 188240968, 288122410, 288098205, 594425589, 477214428, 1073741795, 1073741823),
    (289706568, 45655553, 169102537, 172004250, 2835800, 173302297, 178397747, 353898705, 56170696, 408235085, 105219488, 306655338, 402742464, 45142421, 768410931, 1073741797, 1073741823),
)
ABOVE = (
    (13896576, 673402933, 19091526, 178524557, 675834374, 51990658, 850067701, 306297728, 170449992, 287650507, 405411464, 442805482, 421860451, 457513106, 439203043, 474846434, 1066252059),
    (148151625, 134244928, 103025705, 688149005, 405602480, 44374920, 406106312, 86087593, 52638233, 13542099, 307600534, 55518297, 374712961, 575354083, 340731099, 577357539, 1065985299),
    (20971520, 35709265, 365498738, 845197384, 380436613, 499234072, 347668506, 269323138, 776524186, 348427482, 556634205, 319294346, 342799241, 189486801, 866690931, 159683291, 1065726556),
    (17076224, 17604680, 424436570, 37863598, 816656755, 188748386, 38547883, 438420806, 52506966, 688669934, 432330398, 422652826, 107832665, 365797461, 22647371, 711304514, 1065697958),
)
X_FIRST = (0xffde842a, 0xf44c0150, 0x560b52ff, 0x80058805)
Y_FIRST = (0x216095, 0x28a3, 0xa9f4ad00, 0x74021000)
X_ABOVE = (0x28f58fa2, 0xefff6e08, 0x40e24a, 0x148546be)
Y_ABOVE = (0x14023045, 0x10009084, 0xbb3e0531, 0x6b7ab940)
U_ABOVE = (0xc3084018, 0x173, 0x44811884, 0x80000001)
D_FIRST = (0x1b40, 0xbb3d60c, 0x0, 0xbf867fa)


def pick(place, values):
    total = jnp.int32(0)
    for i, v in enumerate(values):
        total = total + jnp.where(place == i, jnp.int32(v), jnp.int32(0))
    return total


def signed(mask):
    return mask - (1 << 32) if mask >= 1 << 31 else mask


def split(x):
    high = x.astype(jnp.bfloat16)
    return high, (x - high.astype(jnp.float32)).astype(jnp.bfloat16)


def kernel(count, rhs, fac, inv, xbuf, sent, fbuf, fraw, ibuf, ihigh, ilow,
           f_in, f_send, f_recv, i_in, x_in,
           own_recv, a_recv, b_recv, d_recv,
           x_send, y_send, next_send, prev_send, rx_send, ry_send, rn_send, rp_send, rd_send):
    chunks, cycles, tile, lanes = xbuf.shape
    panels = inv.shape[0]
    kpart = fac.shape[3]
    size = tile // PARTS
    planes = count // panels
    bf16, f32 = jnp.bfloat16, jnp.float32

    me = lax.axis_index("rows")
    core = lax.axis_index("rhs")
    z = me // panels
    c = me % panels
    n1 = c + 1 - 2 * (c % 2)
    n2 = (c + 2) % panels
    across = panels - 1 - c
    base = z * panels
    to_core = {"rows": me, "rhs": 1 - core}
    to_n1 = {"rows": base + n1, "rhs": core}
    to_n2 = {"rows": base + n2, "rhs": core}
    middle = planes // 2
    solves = z == 0
    source = jnp.where(z == middle, 0, jnp.where(z < middle, z + 1, z - 1))
    to_next = ((z == 0) & (planes > 1)) | ((z >= middle) & (z > 0) & (z < planes - 1))
    to_prev = (z <= middle) & (z > 1)
    next_plane = jnp.where(z == 0, middle, jnp.minimum(z + 1, planes - 1))
    at_next = {"rows": next_plane * panels + c, "rhs": core}
    at_prev = {"rows": jnp.maximum(z - 1, 0) * panels + c, "rhs": core}
    at_source = {"rows": source * panels + c, "rhs": core}
    early = solves & (c == 0)

    at_bottom = {"rows": c, "rhs": core}
    at_first = {"rows": jnp.where(planes > 1, panels, 0) + c, "rhs": core}

    def table(first, above, place):
        return jnp.where(solves, pick(place, first), pick(place, above))

    x_mask = table([signed(m) for m in X_FIRST], [signed(m) for m in X_ABOVE], n1)
    y_mask = table([signed(m) for m in Y_FIRST], [signed(m) for m in Y_ABOVE], n2)
    d_mask = jnp.where(z == 1, pick(c, [signed(m) for m in D_FIRST]), 0)
    u_mask = jnp.where(to_next | to_prev, pick(c, [signed(m) for m in U_ABOVE]), 0)

    def bit(mask, k):
        return (jnp.right_shift(mask, k % 32) & 1) == 1

    def x_load(j):
        cols = pl.ds(pl.multiple_of(j * lanes, lanes), lanes)
        return pltpu.make_async_copy(rhs.at[:, :, cols], xbuf.at[j], x_in.at[j])

    def i_load():
        return pltpu.make_async_copy(inv.at[c], ibuf, i_in)

    def f_load(cycle):
        return pltpu.make_async_copy(fac.at[cycle], fraw.at[cycle], f_in.at[cycle])

    def f_remote(cycle, p, half):
        at = pl.multiple_of(p * 2 * kpart + half * kpart, kpart)
        ref = fbuf.at[pl.ds(cycle * tile, tile), pl.ds(at, kpart)]
        s = cycle * panels + p
        return pltpu.make_async_remote_copy(ref, ref, f_send.at[s], f_recv.at[s], device_id=to_core)

    def f_place(cycle):
        f_load(cycle).wait()
        step = 64

        @pl.loop(0, tile // step)
        def _(i):
            rows = pl.ds(pl.multiple_of(i * step, step), step)
            to = pl.ds(pl.multiple_of(cycle * tile + i * step, step), step)
            block = jnp.transpose(fraw[cycle, rows], (1, 0, 2))
            for p in range(panels):
                at = pl.multiple_of(p * 2 * kpart + core * kpart, kpart)
                fbuf[to, pl.ds(at, kpart)] = block[p]

    def f_share(cycle):
        for p in range(panels):
            f_remote(cycle, p, core).start()

    def hop(p, k, send, recv, to):
        at = pl.multiple_of(p * tile + (k % PARTS) * size, size)
        ref = sent.at[k // PARTS, pl.ds(at, size)]
        return pltpu.make_async_remote_copy(ref, ref, send.at[k], recv.at[k], device_id=to)

    own_x = lambda k: hop(c, k, x_send, a_recv, to_n1)
    own_y = lambda k: hop(c, k, y_send, b_recv, to_n2)
    own_next = lambda k: hop(c, k, next_send, own_recv, at_next)
    own_prev = lambda k: hop(c, k, prev_send, own_recv, at_prev)
    relay_x = lambda k: hop(n2, k, rx_send, d_recv, to_n1)
    relay_y = lambda k: hop(n1, k, ry_send, d_recv, to_n2)
    relay_next = lambda k: hop(across, k, rn_send, d_recv, at_next)
    relay_down = lambda k: hop(across, k, rd_send, d_recv, at_bottom)
    relay_prev = lambda k: hop(across, k, rp_send, d_recv, at_prev)
    arrive_a = lambda k: hop(n1, k, x_send, a_recv, to_n1)
    arrive_b = lambda k: hop(n2, k, y_send, b_recv, to_n2)
    arrive_d = lambda k: hop(across, k, rx_send, d_recv, to_n1)

    barrier = pltpu.get_barrier_semaphore()
    for to in (to_core, to_n1, to_n2):
        pl.semaphore_signal(barrier, inc=1, device_id=to)

    apart = middle > 1
    for on, to in (
        (to_next, at_next), (to_prev, at_prev), (z > 0, at_source),
        (solves & apart, at_first), ((z == 1) & apart, at_bottom),
    ):
        @pl.when(on)
        def _():
            pl.semaphore_signal(barrier, inc=1, device_id=to)

    @pl.when(solves)
    def _():
        i_load().start()

    x_load(0).start()

    def load_rest():
        for cycle in range(cycles):
            f_load(cycle).start()

        @pl.loop(1, chunks)
        def _(j):
            x_load(j).start()

    @pl.when(jnp.logical_not(early))
    def _():
        load_rest()

    def f_wait(cycle):
        for p in range(panels):
            f_remote(cycle, p, 1 - core).wait_recv()

    @pl.when(solves)
    def _():
        i_load().wait()
        high, low = split(ibuf[...])
        ihigh[...] = high
        ilow[...] = low

    def correct(p, j):
        rows = slice(p * tile, (p + 1) * tile)
        delta = jnp.dot(fbuf[:tile, rows], sent[j, rows], preferred_element_type=f32)
        xbuf[j, 0] = xbuf[j, 0] - delta

    def solve(p, j):
        if p == 0:
            x_load(j).wait()
        high, low = split(xbuf[j, 0])
        both = jnp.concatenate([high, low], axis=1)
        block = tile // 2
        for r in range(2):
            rows = slice(r * block, (r + 1) * block)
            depth = (r + 1) * block
            wide = jnp.dot(ihigh[rows, :depth], both[:depth], preferred_element_type=f32)
            rest = jnp.dot(ilow[rows, :depth], high[:depth], preferred_element_type=f32)
            solved = rest + wide[:, lanes:] + wide[:, :lanes]
            sent[j, p * tile + r * block:p * tile + (r + 1) * block] = solved.astype(bf16)
            xbuf[j, 0, rows] = solved

    @pl.when(early)
    def _():
        solve(0, 0)
        load_rest()

    @pl.when(jnp.logical_not(early))
    def _():
        for cycle in range(cycles):
            f_place(cycle)

    words = [table([row[w] for row in FIRST], [row[w] for row in ABOVE], c) for w in range(len(FIRST[0]))]
    pl.semaphore_wait(
        barrier,
        3 + jnp.where(to_next, 1, 0) + jnp.where(to_prev, 1, 0) + jnp.where(z > 0, 1, 0)
        + jnp.where((z < 2) & apart, 1, 0),
    )

    @pl.when(jnp.logical_not(early))
    def _():
        for cycle in range(cycles):
            f_share(cycle)

        @pl.loop(0, chunks)
        def _(j):
            x_load(j).wait()

    @pl.when(solves & (c > 0))
    def _():
        f_wait(0)

    def take(p, k):
        @pl.when(p == c)
        def _():
            @pl.when(solves)
            def _():
                if p == 0:
                    @pl.when(k > 0)
                    def _():
                        solve(p, k // PARTS)
                else:
                    solve(p, k // PARTS)

                @pl.when(to_next)
                def _():
                    for i in range(PARTS):
                        own_next(k + i).start()

                if p == 0:
                    @pl.when(k == 3 * PARTS)
                    def _():
                        for cycle in range(cycles):
                            f_place(cycle)
                        for cycle in range(cycles):
                            f_share(cycle)

            @pl.when(z > 0)
            def _():
                own_next(k).wait_recv()

                @pl.when(to_next)
                def _():
                    own_next(k).start()

                @pl.when(to_prev)
                def _():
                    own_prev(k).start()

        @pl.when(p == n1)
        def _():
            arrive_a(k).wait_recv()

            @pl.when(bit(y_mask, k))
            def _():
                relay_y(k).start()

        @pl.when(p == n2)
        def _():
            arrive_b(k).wait_recv()

            @pl.when(bit(x_mask, k))
            def _():
                relay_x(k).start()

        @pl.when(p == across)
        def _():
            arrive_d(k).wait_recv()

            @pl.when(bit(u_mask, k) & to_next)
            def _():
                relay_next(k).start()

            @pl.when(bit(u_mask, k) & to_prev)
            def _():
                relay_prev(k).start()

            @pl.when(bit(d_mask, k))
            def _():
                relay_down(k).start()

        @pl.when(solves & (p < c) & (k % PARTS == PARTS - 1))
        def _():
            correct(p, k // PARTS)

    def drain(k):
        @pl.when(to_next)
        def _():
            own_next(k).wait_send()

        @pl.when(to_prev)
        def _():
            own_prev(k).wait_send()

        @pl.when(bit(x_mask, k))
        def _():
            relay_x(k).wait_send()

        @pl.when(bit(y_mask, k))
        def _():
            relay_y(k).wait_send()

        @pl.when(bit(u_mask, k) & to_next)
        def _():
            relay_next(k).wait_send()

        @pl.when(bit(u_mask, k) & to_prev)
        def _():
            relay_prev(k).wait_send()

        @pl.when(bit(d_mask, k))
        def _():
            relay_down(k).wait_send()

    def update(u):
        @pl.when(u == 0)
        def _():
            f_wait(1)

            @pl.when((z > 0) | (c == 0))
            def _():
                f_wait(0)

        @pl.loop(jnp.where(solves, 1, 0), cycles)
        def _(cycle):
            rows = pl.ds(pl.multiple_of(cycle * tile, tile), tile)
            both = jnp.concatenate([sent[2 * u], sent[2 * u + 1]], axis=1)
            delta = jnp.dot(fbuf[rows, :], both, preferred_element_type=f32)
            xbuf[2 * u, cycle] = xbuf[2 * u, cycle] - delta[:, :lanes]
            xbuf[2 * u + 1, cycle] = xbuf[2 * u + 1, cycle] - delta[:, lanes:]

    def step(_, state):
        word, at, xs, ys, us = state
        symbol = word & 7

        for p in range(panels):
            @pl.when(symbol == p)
            def _():
                take(p, at[p])

        @pl.when((symbol == 4) & (us > 1))
        def _():
            @pl.loop(0, 2 * PARTS)
            def _(i):
                drain((us - 2) * 2 * PARTS + i)

        @pl.when((symbol == 4) & (us < chunks // 2 - 1))
        def _():
            update(us)

        @pl.when(symbol == 5)
        def _():
            for i in range(PARTS):
                own_x(PARTS * xs + i).start()

        @pl.when(symbol == 6)
        def _():
            for i in range(PARTS):
                own_y(PARTS * ys + i).start()

        at = tuple(
            a + jnp.where(symbol == p, jnp.where(solves & (c == p), PARTS, 1), 0) for p, a in enumerate(at)
        )
        xs = xs + jnp.where(symbol == 5, 1, 0)
        ys = ys + jnp.where(symbol == 6, 1, 0)
        us = us + jnp.where(symbol == 4, 1, 0)
        return jnp.right_shift(word, 3), at, xs, ys, us

    def stride(w, state):
        word = pick(w, [0] * 0)
        for i, value in enumerate(words):
            word = word + jnp.where(w == i, value, 0)
        return lax.fori_loop(0, SHARE, step, (word,) + state)[1:]

    zero = jnp.int32(0)
    lax.fori_loop(0, len(words), stride, ((zero,) * panels, zero, zero, zero))

    @pl.loop(0, chunks * PARTS)
    def _(k):
        own_x(k).wait_send()
        own_y(k).wait_send()

    @pl.loop((chunks - 4) * PARTS, chunks * PARTS)
    def _(k):
        drain(k)

    for cycle in range(cycles):
        for p in range(panels):
            f_remote(cycle, p, core).wait_send()


def finish(panels, xbuf, sent, fbuf, out, last, sems):
    chunks, cycles, tile, lanes = xbuf.shape
    first = chunks - 2
    solves = lax.axis_index("rows") < panels

    def store(j, ref):
        cols = pl.ds(pl.multiple_of(j * lanes, lanes), lanes)
        return pltpu.make_async_copy(ref, out.at[:, :, cols], sems.at[j])

    @pl.loop(0, first)
    def _(j):
        store(j, xbuf.at[j]).start()

    @pl.when(solves)
    def _():
        last[:, 0] = xbuf[first:, 0]

    both = jnp.concatenate([sent[first], sent[first + 1]], axis=1)

    @pl.loop(jnp.where(solves, 1, 0), cycles)
    def _(cycle):
        rows = pl.ds(pl.multiple_of(cycle * tile, tile), tile)
        delta = jnp.dot(fbuf[rows, :], both, preferred_element_type=jnp.float32)
        last[0, cycle] = xbuf[first, cycle] - delta[:, :lanes]
        last[1, cycle] = xbuf[first + 1, cycle] - delta[:, lanes:]

    for i in range(2):
        store(first + i, last.at[i]).start()

    @pl.loop(0, chunks)
    def _(j):
        store(j, xbuf.at[j]).wait()


def local(rhs, factor, inverses):
    count = lax.axis_size("rows")
    cycles, tile, width = rhs.shape
    panels = inverses.shape[0]
    kpart = factor.shape[3]
    chunks = width // LANES
    units = chunks * PARTS
    bf16, f32 = jnp.bfloat16, jnp.float32
    dma = lambda n: pltpu.SemaphoreType.DMA((n,))
    vmem = pl.BlockSpec(memory_space=pltpu.VMEM)
    state = pl.pallas_call(
        functools.partial(kernel, count),
        out_shape=(
            pltpu.VMEM((chunks, cycles, tile, LANES), f32),
            pltpu.VMEM((chunks, panels * tile, LANES), bf16),
            pltpu.VMEM((cycles * tile, panels * tile), bf16),
        ),
        in_specs=[pl.BlockSpec(memory_space=pltpu.HBM)] * 3,
        out_specs=(vmem, vmem, vmem),
        scratch_shapes=[
            pltpu.VMEM(factor.shape, bf16),
            pltpu.VMEM((tile, tile), f32),
            pltpu.VMEM((tile, tile), bf16),
            pltpu.VMEM((tile, tile), bf16),
            dma(cycles), dma(cycles * panels), dma(cycles * panels),
            pltpu.SemaphoreType.DMA, dma(chunks),
        ] + [dma(units)] * 13,
        compiler_params=pltpu.CompilerParams(
            collective_id=0, has_side_effects=True, vmem_limit_bytes=43 << 20
        ),
        name="substitute",
    )(rhs, factor, inverses)
    return pl.pallas_call(
        functools.partial(finish, panels),
        out_shape=jax.ShapeDtypeStruct(rhs.shape, f32),
        in_specs=[vmem] * 3,
        out_specs=pl.BlockSpec(memory_space=pl.ANY),
        scratch_shapes=[pltpu.VMEM((2, cycles, tile, LANES), f32), dma(chunks)],
        compiler_params=pltpu.CompilerParams(vmem_limit_bytes=16 << 20),
        name="finish",
    )(*state)


def solution(mesh):
    return jax.shard_map(
        local,
        mesh=mesh,
        in_specs=(P(None, "rows", "rhs"), P(None, "rows", None, "rhs"), P()),
        out_specs=P(None, "rows", "rhs"),
        check_vma=False,
    )
```

```python
import functools

import jax
import jax.numpy as jnp
from jax import lax
from jax.experimental import pallas as pl
from jax.experimental.pallas import tpu as pltpu
from jax.sharding import PartitionSpec as P

LANES = 128
PARTS = 2
SHARE = 10
FIRST = (
    (111366568, 152621109, 152621453, 178594189, 136741718, 105489006, 463672147, 154412425, 437818515, 826594450, 423182930, 309184147, 325960858, 460211931, 594396315, 1073741795, 1073741823),
    (891316800, 891316800, 891507200, 138504768, 11306542, 421179507, 414746501, 407735176, 319399281, 459926082, 460184640, 308913947, 342733979, 340337812, 306783508, 1073741796, 1073741823),
    (134479872, 839130000, 144908813, 410313792, 438668177, 833130924, 285490065, 35757277, 271353768, 893766749, 188240968, 288122410, 288098205, 594425589, 477214428, 1073741795, 1073741823),
    (289706568, 45655553, 169102537, 172004250, 2835800, 173302297, 178397747, 353898705, 56170696, 408235085, 105219488, 306655338, 402742464, 45142421, 768410931, 1073741797, 1073741823),
)
ABOVE = (
    (13896576, 673402933, 19091526, 178524557, 675834374, 51990658, 850067701, 306297728, 170449992, 287650507, 405411464, 442805482, 421860451, 457513106, 439203043, 474846434, 1066252059),
    (148151625, 134244928, 103025705, 688149005, 405602480, 44374920, 406106312, 86087593, 52638233, 13542099, 307600534, 55518297, 374712961, 575354083, 340731099, 577357539, 1065985299),
    (20971520, 35709265, 365498738, 845197384, 380436613, 499234072, 347668506, 269323138, 776524186, 348427482, 556634205, 319294346, 342799241, 189486801, 866690931, 159683291, 1065726556),
    (17076224, 17604680, 424436570, 37863598, 816656755, 188748386, 38547883, 438420806, 52506966, 688669934, 432330398, 422652826, 107832665, 365797461, 22647371, 711304514, 1065697958),
)
X_FIRST = (0xffde842a, 0xf44c0150, 0x560b52ff, 0x80058805)
Y_FIRST = (0x216095, 0x28a3, 0xa9f4ad00, 0x74021000)
X_ABOVE = (0x28f58fa2, 0xefff6e08, 0x40e24a, 0x148546be)
Y_ABOVE = (0x14023045, 0x10009084, 0xbb3e0531, 0x6b7ab940)
U_ABOVE = (0xc3084018, 0x173, 0x44811884, 0x80000001)
D_FIRST = (0x1b40, 0xbb3d60c, 0x0, 0xbf867fa)


def pick(place, values):
    total = jnp.int32(0)
    for i, v in enumerate(values):
        total = total + jnp.where(place == i, jnp.int32(v), jnp.int32(0))
    return total


def signed(mask):
    return mask - (1 << 32) if mask >= 1 << 31 else mask


def split(x):
    high = x.astype(jnp.bfloat16)
    return high, (x - high.astype(jnp.float32)).astype(jnp.bfloat16)


def kernel(count, rhs, fac, inv, xbuf, sent, fbuf, fraw, ibuf, ihigh, ilow,
           f_in, f_send, f_recv, i_in, x_in,
           own_recv, a_recv, b_recv, d_recv,
           x_send, y_send, next_send, prev_send, rx_send, ry_send, rn_send, rp_send, rd_send):
    chunks, cycles, tile, lanes = xbuf.shape
    panels = inv.shape[0]
    kpart = fac.shape[3]
    size = tile // PARTS
    planes = count // panels
    bf16, f32 = jnp.bfloat16, jnp.float32

    me = lax.axis_index("rows")
    core = lax.axis_index("rhs")
    z = me // panels
    c = me % panels
    n1 = c + 1 - 2 * (c % 2)
    n2 = (c + 2) % panels
    across = panels - 1 - c
    base = z * panels
    to_core = {"rows": me, "rhs": 1 - core}
    to_n1 = {"rows": base + n1, "rhs": core}
    to_n2 = {"rows": base + n2, "rhs": core}
    middle = planes // 2
    solves = z == 0
    source = jnp.where(z == middle, 0, jnp.where(z < middle, z + 1, z - 1))
    to_next = ((z == 0) & (planes > 1)) | ((z >= middle) & (z > 0) & (z < planes - 1))
    to_prev = (z <= middle) & (z > 1)
    next_plane = jnp.where(z == 0, middle, jnp.minimum(z + 1, planes - 1))
    at_next = {"rows": next_plane * panels + c, "rhs": core}
    at_prev = {"rows": jnp.maximum(z - 1, 0) * panels + c, "rhs": core}
    at_source = {"rows": source * panels + c, "rhs": core}
    early = solves & (c == 0)

    at_bottom = {"rows": c, "rhs": core}
    at_first = {"rows": jnp.where(planes > 1, panels, 0) + c, "rhs": core}

    def table(first, above, place):
        return jnp.where(solves, pick(place, first), pick(place, above))

    x_mask = table([signed(m) for m in X_FIRST], [signed(m) for m in X_ABOVE], n1)
    y_mask = table([signed(m) for m in Y_FIRST], [signed(m) for m in Y_ABOVE], n2)
    d_mask = jnp.where(z == 1, pick(c, [signed(m) for m in D_FIRST]), 0)
    u_mask = jnp.where(to_next | to_prev, pick(c, [signed(m) for m in U_ABOVE]), 0)

    def bit(mask, k):
        return (jnp.right_shift(mask, k % 32) & 1) == 1

    def x_load(j):
        cols = pl.ds(pl.multiple_of(j * lanes, lanes), lanes)
        return pltpu.make_async_copy(rhs.at[:, :, cols], xbuf.at[j], x_in.at[j])

    def i_load():
        return pltpu.make_async_copy(inv.at[c], ibuf, i_in)

    def f_load(cycle):
        return pltpu.make_async_copy(fac.at[cycle], fraw.at[cycle], f_in.at[cycle])

    def f_remote(cycle, p, half):
        at = pl.multiple_of(p * 2 * kpart + half * kpart, kpart)
        ref = fbuf.at[pl.ds(cycle * tile, tile), pl.ds(at, kpart)]
        s = cycle * panels + p
        return pltpu.make_async_remote_copy(ref, ref, f_send.at[s], f_recv.at[s], device_id=to_core)

    def f_place(cycle):
        f_load(cycle).wait()
        step = 64

        @pl.loop(0, tile // step)
        def _(i):
            rows = pl.ds(pl.multiple_of(i * step, step), step)
            to = pl.ds(pl.multiple_of(cycle * tile + i * step, step), step)
            block = jnp.transpose(fraw[cycle, rows], (1, 0, 2))
            for p in range(panels):
                at = pl.multiple_of(p * 2 * kpart + core * kpart, kpart)
                fbuf[to, pl.ds(at, kpart)] = block[p]

    def f_share(cycle):
        for p in range(panels):
            f_remote(cycle, p, core).start()

    def hop(p, k, send, recv, to):
        at = pl.multiple_of(p * tile + (k % PARTS) * size, size)
        ref = sent.at[k // PARTS, pl.ds(at, size)]
        return pltpu.make_async_remote_copy(ref, ref, send.at[k], recv.at[k], device_id=to)

    own_x = lambda k: hop(c, k, x_send, a_recv, to_n1)
    own_y = lambda k: hop(c, k, y_send, b_recv, to_n2)
    own_next = lambda k: hop(c, k, next_send, own_recv, at_next)
    own_prev = lambda k: hop(c, k, prev_send, own_recv, at_prev)
    relay_x = lambda k: hop(n2, k, rx_send, d_recv, to_n1)
    relay_y = lambda k: hop(n1, k, ry_send, d_recv, to_n2)
    relay_next = lambda k: hop(across, k, rn_send, d_recv, at_next)
    relay_down = lambda k: hop(across, k, rd_send, d_recv, at_bottom)
    relay_prev = lambda k: hop(across, k, rp_send, d_recv, at_prev)
    arrive_a = lambda k: hop(n1, k, x_send, a_recv, to_n1)
    arrive_b = lambda k: hop(n2, k, y_send, b_recv, to_n2)
    arrive_d = lambda k: hop(across, k, rx_send, d_recv, to_n1)

    barrier = pltpu.get_barrier_semaphore()
    for to in (to_core, to_n1, to_n2):
        pl.semaphore_signal(barrier, inc=1, device_id=to)

    apart = middle > 1
    for on, to in (
        (to_next, at_next), (to_prev, at_prev), (z > 0, at_source),
        (solves & apart, at_first), ((z == 1) & apart, at_bottom),
    ):
        @pl.when(on)
        def _():
            pl.semaphore_signal(barrier, inc=1, device_id=to)

    @pl.when(solves)
    def _():
        i_load().start()

    x_load(0).start()

    def load_rest():
        for cycle in range(cycles):
            f_load(cycle).start()

        @pl.loop(1, chunks)
        def _(j):
            x_load(j).start()

    @pl.when(jnp.logical_not(early))
    def _():
        load_rest()

    def f_wait(cycle):
        for p in range(panels):
            f_remote(cycle, p, 1 - core).wait_recv()

    @pl.when(solves)
    def _():
        i_load().wait()
        high, low = split(ibuf[...])
        ihigh[...] = high
        ilow[...] = low

    def correct(p, j):
        rows = slice(p * tile, (p + 1) * tile)
        delta = jnp.dot(fbuf[:tile, rows], sent[j, rows], preferred_element_type=f32)
        xbuf[j, 0] = xbuf[j, 0] - delta

    def solve(p, j):
        if p == 0:
            x_load(j).wait()
        high, low = split(xbuf[j, 0])
        both = jnp.concatenate([high, low], axis=1)
        block = tile // 2
        for r in range(2):
            rows = slice(r * block, (r + 1) * block)
            depth = (r + 1) * block
            wide = jnp.dot(ihigh[rows, :depth], both[:depth], preferred_element_type=f32)
            rest = jnp.dot(ilow[rows, :depth], high[:depth], preferred_element_type=f32)
            solved = rest + wide[:, lanes:] + wide[:, :lanes]
            sent[j, p * tile + r * block:p * tile + (r + 1) * block] = solved.astype(bf16)
            xbuf[j, 0, rows] = solved

    @pl.when(early)
    def _():
        solve(0, 0)
        load_rest()

    @pl.when(jnp.logical_not(early))
    def _():
        for cycle in range(cycles):
            f_place(cycle)

    words = [table([row[w] for row in FIRST], [row[w] for row in ABOVE], c) for w in range(len(FIRST[0]))]
    pl.semaphore_wait(
        barrier,
        3 + jnp.where(to_next, 1, 0) + jnp.where(to_prev, 1, 0) + jnp.where(z > 0, 1, 0)
        + jnp.where((z < 2) & apart, 1, 0),
    )

    @pl.when(jnp.logical_not(early))
    def _():
        for cycle in range(cycles):
            f_share(cycle)

        @pl.loop(0, chunks)
        def _(j):
            x_load(j).wait()

    @pl.when(solves & (c > 0))
    def _():
        f_wait(0)

    def take(p, k):
        @pl.when(p == c)
        def _():
            @pl.when(solves)
            def _():
                if p == 0:
                    @pl.when(k > 0)
                    def _():
                        solve(p, k // PARTS)
                else:
                    solve(p, k // PARTS)

                @pl.when(to_next)
                def _():
                    for i in range(PARTS):
                        own_next(k + i).start()

                if p == 0:
                    @pl.when(k == 3 * PARTS)
                    def _():
                        for cycle in range(cycles):
                            f_place(cycle)
                        for cycle in range(cycles):
                            f_share(cycle)

            @pl.when(z > 0)
            def _():
                own_next(k).wait_recv()

                @pl.when(to_next)
                def _():
                    own_next(k).start()

                @pl.when(to_prev)
                def _():
                    own_prev(k).start()

        @pl.when(p == n1)
        def _():
            arrive_a(k).wait_recv()

            @pl.when(bit(y_mask, k))
            def _():
                relay_y(k).start()

        @pl.when(p == n2)
        def _():
            arrive_b(k).wait_recv()

            @pl.when(bit(x_mask, k))
            def _():
                relay_x(k).start()

        @pl.when(p == across)
        def _():
            arrive_d(k).wait_recv()

            @pl.when(bit(u_mask, k) & to_next)
            def _():
                relay_next(k).start()

            @pl.when(bit(u_mask, k) & to_prev)
            def _():
                relay_prev(k).start()

            @pl.when(bit(d_mask, k))
            def _():
                relay_down(k).start()

        @pl.when(solves & (p < c) & (k % PARTS == PARTS - 1))
        def _():
            correct(p, k // PARTS)

    def drain(k):
        own_x(k).wait_send()
        own_y(k).wait_send()

        @pl.when(to_next)
        def _():
            own_next(k).wait_send()

        @pl.when(to_prev)
        def _():
            own_prev(k).wait_send()

        @pl.when(bit(x_mask, k))
        def _():
            relay_x(k).wait_send()

        @pl.when(bit(y_mask, k))
        def _():
            relay_y(k).wait_send()

        @pl.when(bit(u_mask, k) & to_next)
        def _():
            relay_next(k).wait_send()

        @pl.when(bit(u_mask, k) & to_prev)
        def _():
            relay_prev(k).wait_send()

        @pl.when(bit(d_mask, k))
        def _():
            relay_down(k).wait_send()

    def update(u):
        @pl.when(u == 0)
        def _():
            f_wait(1)

            @pl.when((z > 0) | (c == 0))
            def _():
                f_wait(0)

        @pl.loop(jnp.where(solves, 1, 0), cycles)
        def _(cycle):
            rows = pl.ds(pl.multiple_of(cycle * tile, tile), tile)
            both = jnp.concatenate([sent[2 * u], sent[2 * u + 1]], axis=1)
            delta = jnp.dot(fbuf[rows, :], both, preferred_element_type=f32)
            xbuf[2 * u, cycle] = xbuf[2 * u, cycle] - delta[:, :lanes]
            xbuf[2 * u + 1, cycle] = xbuf[2 * u + 1, cycle] - delta[:, lanes:]

    def step(_, state):
        word, at, xs, ys, us = state
        symbol = word & 7

        for p in range(panels):
            @pl.when(symbol == p)
            def _():
                take(p, at[p])

        @pl.when((symbol == 4) & (us > 1))
        def _():
            @pl.loop(0, 2 * PARTS)
            def _(i):
                drain((us - 2) * 2 * PARTS + i)

        @pl.when((symbol == 4) & (us < chunks // 2 - 1))
        def _():
            update(us)

        @pl.when(symbol == 5)
        def _():
            for i in range(PARTS):
                own_x(PARTS * xs + i).start()

        @pl.when(symbol == 6)
        def _():
            for i in range(PARTS):
                own_y(PARTS * ys + i).start()

        at = tuple(
            a + jnp.where(symbol == p, jnp.where(solves & (c == p), PARTS, 1), 0) for p, a in enumerate(at)
        )
        xs = xs + jnp.where(symbol == 5, 1, 0)
        ys = ys + jnp.where(symbol == 6, 1, 0)
        us = us + jnp.where(symbol == 4, 1, 0)
        return jnp.right_shift(word, 3), at, xs, ys, us

    def stride(w, state):
        word = pick(w, [0] * 0)
        for i, value in enumerate(words):
            word = word + jnp.where(w == i, value, 0)
        return lax.fori_loop(0, SHARE, step, (word,) + state)[1:]

    zero = jnp.int32(0)
    lax.fori_loop(0, len(words), stride, ((zero,) * panels, zero, zero, zero))

    @pl.loop((chunks - 4) * PARTS, chunks * PARTS)
    def _(k):
        drain(k)

    for cycle in range(cycles):
        for p in range(panels):
            f_remote(cycle, p, core).wait_send()


def finish(panels, xbuf, sent, fbuf, out, last, sems):
    chunks, cycles, tile, lanes = xbuf.shape
    first = chunks - 2
    solves = lax.axis_index("rows") < panels

    def store(j, ref):
        cols = pl.ds(pl.multiple_of(j * lanes, lanes), lanes)
        return pltpu.make_async_copy(ref, out.at[:, :, cols], sems.at[j])

    @pl.loop(0, first)
    def _(j):
        store(j, xbuf.at[j]).start()

    @pl.when(solves)
    def _():
        last[:, 0] = xbuf[first:, 0]

    both = jnp.concatenate([sent[first], sent[first + 1]], axis=1)

    @pl.loop(jnp.where(solves, 1, 0), cycles)
    def _(cycle):
        rows = pl.ds(pl.multiple_of(cycle * tile, tile), tile)
        delta = jnp.dot(fbuf[rows, :], both, preferred_element_type=jnp.float32)
        last[0, cycle] = xbuf[first, cycle] - delta[:, :lanes]
        last[1, cycle] = xbuf[first + 1, cycle] - delta[:, lanes:]

    for i in range(2):
        store(first + i, last.at[i]).start()

    @pl.loop(0, chunks)
    def _(j):
        store(j, xbuf.at[j]).wait()


def local(rhs, factor, inverses):
    count = lax.axis_size("rows")
    cycles, tile, width = rhs.shape
    panels = inverses.shape[0]
    kpart = factor.shape[3]
    chunks = width // LANES
    units = chunks * PARTS
    bf16, f32 = jnp.bfloat16, jnp.float32
    dma = lambda n: pltpu.SemaphoreType.DMA((n,))
    vmem = pl.BlockSpec(memory_space=pltpu.VMEM)
    state = pl.pallas_call(
        functools.partial(kernel, count),
        out_shape=(
            pltpu.VMEM((chunks, cycles, tile, LANES), f32),
            pltpu.VMEM((chunks, panels * tile, LANES), bf16),
            pltpu.VMEM((cycles * tile, panels * tile), bf16),
        ),
        in_specs=[pl.BlockSpec(memory_space=pltpu.HBM)] * 3,
        out_specs=(vmem, vmem, vmem),
        scratch_shapes=[
            pltpu.VMEM(factor.shape, bf16),
            pltpu.VMEM((tile, tile), f32),
            pltpu.VMEM((tile, tile), bf16),
            pltpu.VMEM((tile, tile), bf16),
            dma(cycles), dma(cycles * panels), dma(cycles * panels),
            pltpu.SemaphoreType.DMA, dma(chunks),
        ] + [dma(units)] * 13,
        compiler_params=pltpu.CompilerParams(
            collective_id=0, has_side_effects=True, vmem_limit_bytes=43 << 20
        ),
        name="substitute",
    )(rhs, factor, inverses)
    return pl.pallas_call(
        functools.partial(finish, panels),
        out_shape=jax.ShapeDtypeStruct(rhs.shape, f32),
        in_specs=[vmem] * 3,
        out_specs=pl.BlockSpec(memory_space=pl.ANY),
        scratch_shapes=[pltpu.VMEM((2, cycles, tile, LANES), f32), dma(chunks)],
        compiler_params=pltpu.CompilerParams(vmem_limit_bytes=16 << 20),
        name="finish",
    )(*state)


def solution(mesh):
    return jax.shard_map(
        local,
        mesh=mesh,
        in_specs=(P(None, "rows", "rhs"), P(None, "rows", None, "rhs"), P()),
        out_specs=P(None, "rows", "rhs"),
        check_vma=False,
    )
```
